128 devices in a mesh: node: 128 (over y, z, x, core).
Axes of the slice: x: 4, y: 4, z: 4, core: 2. Of those that a mesh axis runs over, the one named last changes fastest.
Arguments:
- node_feats: bfloat16 [131072, 128], P('node'), may hold values from -240 to 240
- weight: bfloat16 [128, 128], replicated, may hold values from -0.5 to 0.5
- att_src: float32 [8, 16], replicated, may hold values from -1.5 to 1.5
- att_dst: float32 [8, 16], replicated, may hold values from -1.5 to 1.5
- out_bias: float32 [128], replicated, may hold values from -3 to 3
- requests: int32 [128, 128], P('node'), may hold values from 0 to 7
- tile_dst: int32 [128, 128], P('node'), may hold values from 0 to 7, as said below
- tile_src: int32 [128, 128], P('node'), may hold values from 0 to 127
- tile_masks: int32 [128, 128, 128, 128], P('node'), may hold values from 0 to 1
- tile_count: int32 [128], P('node'), may hold values from 16 to 128, as said below
Outputs:
- node_out: bfloat16 [131072, 128], P('node')
The draws below stay inside these ranges and needn't reach their ends.
Inputs may be any that keep to these rules, and one draw needn't show every extreme that they name: Within one device the pairs (tile_dst, tile_src) of its 128 slots are distinct. `tile_count`: slots at or past a device's count are unused; some device uses all 128.
All inputs are finite; a program needn't handle non-finite values.
Results may differ from the reference program's by a relative error of at most 0.012.
Values may be sent and summed in bfloat16 or wider, within the bound.
No kernel may reach another device: no remote copies, remote signals or barrier semaphores. Data moves between devices by JAX's collectives and lax.ppermute only.
A program may use at most 128 MiB of HBM per device.

```python
import math
import jax
import jax.numpy as jnp
from jax import lax

HEADS = 8
HD = 16
F = 128
BLK = 128
BLK_DEV = 8
TILES = 128
NODES = 131072
N_NODE = 128


def draw_node_feats(key, part):
    key_a = jax.random.fold_in(jax.random.fold_in(key, 5), 0)
    base_draw = jax.random.truncated_normal(key_a, -6.0, 6.0, (NODES, F), jnp.float32)
    return base_draw.astype(jnp.bfloat16)


def tile_pairs(key):
    sub_keys = jax.random.split(jax.random.fold_in(key, 11), N_NODE)
    pairs = jax.vmap(lambda sub_key: jax.random.permutation(sub_key, BLK_DEV * N_NODE)[:TILES])(sub_keys)
    return pairs.astype(jnp.int32)


def draw_tile_dst(key, part):
    return (tile_pairs(key) // N_NODE).astype(jnp.int32)


def draw_tile_src(key, part):
    return (tile_pairs(key) % N_NODE).astype(jnp.int32)


def draw_tile_masks(key, part):
    key_a, key_b = jax.random.split(jax.random.fold_in(key, 23))
    levels = jax.random.randint(key_a, (N_NODE, TILES, 1, 1), 10, 400)
    coins = jax.random.randint(key_b, (N_NODE, TILES, BLK, BLK), 0, 1000)
    return (coins < levels).astype(jnp.int32)


def draw_tile_count(key, part):
    key_a, key_b = jax.random.split(jax.random.fold_in(key, 31))
    levels = jax.random.randint(key_a, (N_NODE,), 0, 4)
    counts = jnp.right_shift(jnp.full((N_NODE,), TILES, jnp.int32), levels)
    busiest = jax.random.randint(key_b, (1,), 0, N_NODE)
    return jnp.where(jnp.arange(N_NODE) == busiest, TILES, counts).astype(jnp.int32)


def place_ends(result, stream_key, least, largest):
    dims = result.shape
    spot = [jax.random.randint(jax.random.fold_in(stream_key, axis), (), 0, dims[axis]) for axis in range(len(dims))]
    result = result.at[tuple(spot)].set(least)
    longest = dims.index(max(dims))
    spot[longest] = (spot[longest] + 1) % dims[longest]
    return result.at[tuple(spot)].set(largest)


def normal_values(rng, dims, width, limit, kind=jnp.bfloat16):
    return jnp.clip(width * jax.random.normal(rng, dims, jnp.float32), -limit, limit).astype(kind)


def setup_inputs(seed: int = 0) -> dict:
    key_of = jax.random.split(jax.random.key(seed), 11)
    return {
        "node_feats": draw_node_feats(jax.random.fold_in(key_of[10], 71), 0),
        "weight": normal_values(key_of[1], (F, F), F ** -0.5, 0.5),
        "att_src": normal_values(key_of[2], (HEADS, HD), HD ** -0.5, 1.5, jnp.float32),
        "att_dst": normal_values(key_of[3], (HEADS, HD), HD ** -0.5, 1.5, jnp.float32),
        "out_bias": normal_values(key_of[4], (F,), 0.5, 3.0, jnp.float32),
        "requests": place_ends(jax.random.randint(key_of[5], (N_NODE, N_NODE), 0, BLK_DEV), jax.random.fold_in(key_of[5], 1), 0, BLK_DEV - 1).astype(jnp.int32),
        "tile_dst": draw_tile_dst(jax.random.fold_in(key_of[10], 71), 0),
        "tile_src": draw_tile_src(jax.random.fold_in(key_of[10], 71), 0),
        "tile_masks": draw_tile_masks(jax.random.fold_in(key_of[10], 71), 0),
        "tile_count": draw_tile_count(jax.random.fold_in(key_of[10], 71), 0),
    }


def leaky_relu(in_value):
    return jnp.where(in_value > 0, in_value, 0.2 * in_value)


def head_scores(projected, att_vec):
    head_count, head_width = att_vec.shape
    wide_heads = projected.astype(jnp.float32).reshape(projected.shape[0], head_count, head_width)
    return jnp.sum(wide_heads * att_vec, axis=-1)


def by_block(scores, block_size):
    row_count, head_count = scores.shape
    return jnp.transpose(scores.reshape(row_count // block_size, block_size, head_count), (0, 2, 1))


def attend_tiles(own_proj, own_src, own_dst, far_proj, far_src, tile_dst, tile_src, tile_mask, live_count, group_size, out_bias):
    num_blocks, block_size, feat_width = own_proj.shape
    head_count = own_src.shape[1]
    head_width = feat_width // head_count
    self_logit = leaky_relu(own_dst + own_src)
    block_ids = jnp.arange(num_blocks, dtype=jnp.int32)
    rounds = (live_count + group_size - 1) // group_size

    def group_terms(step_index):
        first_tile = (step_index * group_size).astype(jnp.int32)
        dst_ids = lax.dynamic_slice_in_dim(tile_dst, first_tile, group_size, 0)
        src_ids = lax.dynamic_slice_in_dim(tile_src, first_tile, group_size, 0)
        edge_mask = lax.dynamic_slice_in_dim(tile_mask, first_tile, group_size, 0)
        is_live = (first_tile + jnp.arange(group_size, dtype=jnp.int32)) < live_count
        dst_term = jnp.take(own_dst, dst_ids, axis=0)
        src_term = jnp.take(far_src, src_ids, axis=0)
        logits = leaky_relu(dst_term[:, :, :, None] + src_term[:, :, None, :])
        kept_edge = ((edge_mask > 0) & is_live[:, None, None])[:, None]
        one_hot = dst_ids[:, None] == block_ids[None, :]
        return dst_ids, src_ids, logits, kept_edge, one_hot

    def max_step(step_index, row_peak):
        dst_ids, src_ids, logits, kept_edge, one_hot = group_terms(step_index)
        tile_max = jnp.max(jnp.where(kept_edge, logits, -jnp.inf), axis=-1)
        candidate = jnp.max(jnp.where(one_hot[:, :, None, None], tile_max[:, None], -jnp.inf), axis=0)
        return jnp.maximum(row_peak, candidate)

    row_peak = lax.fori_loop(0, rounds, max_step, self_logit)
    self_weight = jnp.exp(self_logit - row_peak)
    self_round = lax.optimization_barrier(self_weight.astype(jnp.bfloat16)).astype(jnp.float32)
    own_vals = own_proj.reshape(num_blocks, block_size, head_count, head_width).astype(jnp.float32)
    weighted = jnp.transpose(self_round, (0, 2, 1))[..., None] * own_vals

    def sum_step(step_index, acc_state):
        weighted, norm_sum = acc_state
        dst_ids, src_ids, logits, kept_edge, one_hot = group_terms(step_index)
        row_shift = jnp.take(row_peak, dst_ids, axis=0)
        weights = jnp.exp(jnp.where(kept_edge, logits - row_shift[:, :, :, None], -jnp.inf))
        rounded = weights.astype(jnp.bfloat16).astype(jnp.float32)
        src_vals = jnp.take(far_proj, src_ids, axis=0).reshape(group_size, block_size, head_count, head_width)
        partial_value = jnp.einsum('ghij,gjhd->gihd', rounded, src_vals.astype(jnp.float32))
        pick_mat = one_hot.astype(jnp.float32)
        weighted = weighted + jnp.einsum('gb,gihd->bihd', pick_mat, partial_value, precision=lax.Precision.HIGHEST)
        norm_sum = norm_sum + jnp.einsum('gb,ghi->bhi', pick_mat, jnp.sum(weights, axis=-1), precision=lax.Precision.HIGHEST)
        return weighted, norm_sum

    weighted, norm_sum = lax.fori_loop(0, rounds, sum_step, (weighted, self_weight))
    averaged = weighted / jnp.transpose(norm_sum, (0, 2, 1))[..., None]
    mixed_out = averaged.reshape(num_blocks * block_size, feat_width) + out_bias
    return jax.nn.elu(mixed_out).astype(jnp.bfloat16)


def reference(node_feats, weight, att_src, att_dst, out_bias, requests, tile_dst, tile_src, tile_masks, tile_count):
    projected = jnp.dot(node_feats, weight, preferred_element_type=jnp.float32).astype(jnp.bfloat16)
    proj_blocks = projected.reshape(NODES // BLK, BLK, F)
    src_blocks = by_block(head_scores(projected, att_src), BLK)
    dst_blocks = by_block(head_scores(projected, att_dst), BLK)
    group_size = math.gcd(TILES, 16)
    peer_ids = jnp.arange(N_NODE, dtype=jnp.int32)

    def one_device(device):
        wanted = peer_ids * BLK_DEV + requests[device].astype(jnp.int32)
        far_proj = jnp.take(proj_blocks, wanted, axis=0)
        far_src = jnp.take(src_blocks, wanted, axis=0)
        first_block = (device * BLK_DEV).astype(jnp.int32)
        own_proj = lax.dynamic_slice_in_dim(proj_blocks, first_block, BLK_DEV, 0)
        own_src = lax.dynamic_slice_in_dim(src_blocks, first_block, BLK_DEV, 0)
        own_dst = lax.dynamic_slice_in_dim(dst_blocks, first_block, BLK_DEV, 0)
        return attend_tiles(own_proj, own_src, own_dst, far_proj, far_src, tile_dst[device], tile_src[device], tile_masks[device], tile_count[device], group_size, out_bias)

    results = lax.map(one_device, jnp.arange(N_NODE, dtype=jnp.int32))
    return results.reshape(NODES, F)
```

```python
import jax
import jax.numpy as jnp
from jax import lax
from jax.experimental import pallas as pl
from jax.experimental.pallas import tpu as pltpu
from jax.sharding import PartitionSpec as P

LIMIT = 40.0
GROUP = 16


def split3(table):
    high = lax.reduce_precision(table, 8, 7)
    rest = table - high
    mid = lax.reduce_precision(rest, 8, 7)
    low = rest - mid
    return tuple(part.astype(jnp.bfloat16) for part in (high, mid, low))


def leaky_relu(in_value):
    return jnp.where(in_value > 0, in_value, 0.2 * in_value)


def elu(in_value):
    return jnp.where(in_value > 0, in_value, jnp.exp(jnp.minimum(in_value, 0.0)) - 1.0)


def dot_f32(left, right):
    return jnp.dot(left, right, preferred_element_type=jnp.float32)


def dot_nt(left, right):
    return lax.dot_general(left, right, (((1,), (1,)), ((), ())), preferred_element_type=jnp.float32)


def gather_kernel(wanted_ref, own_ref, out_ref):
    count = out_ref.shape[0]
    first = pl.program_id(0) * count
    for slot in range(count):
        out_ref[slot] = own_ref[wanted_ref[first + slot, 0]]


def gather_blocks(wanted, own_proj):
    peers, lanes = wanted.shape
    num_blocks, rows, feats = own_proj.shape
    step = 16
    return pl.pallas_call(
        gather_kernel,
        grid=(peers // step,),
        in_specs=[
            pl.BlockSpec(memory_space=pltpu.SMEM),
            pl.BlockSpec((num_blocks, rows, feats), lambda g: (0, 0, 0)),
        ],
        out_specs=pl.BlockSpec((step, rows, feats), lambda g: (g, 0, 0)),
        out_shape=jax.ShapeDtypeStruct((peers, rows, feats), own_proj.dtype),
        name="gather_blocks",
    )(wanted, own_proj)


def prep_kernel(own_ref, dst_table_ref, src_exp_ref, dst_exp_ref, ratio_ref, acc_ref, peak_ref):
    own = own_ref[0]
    heads = ratio_ref.shape[1]
    rows = own.shape[0]
    dst_wide = dot_f32(own, dst_table_ref[0]) + dot_f32(own, dst_table_ref[1]) + dot_f32(own, dst_table_ref[2])
    ratio = jnp.exp(-0.8 * dst_wide).astype(jnp.bfloat16)
    for head in range(heads):
        ratio_ref[0, head] = ratio[:, head * rows : (head + 1) * rows]
    src_own = dot_f32(own, src_exp_ref[0]) + dot_f32(own, src_exp_ref[1]) + dot_f32(own, src_exp_ref[2])
    dst_own = dot_f32(own, dst_exp_ref[0]) + dot_f32(own, dst_exp_ref[1]) + dot_f32(own, dst_exp_ref[2])
    self_weight = jnp.maximum(jnp.exp(src_own), jnp.exp(0.2 * src_own - 0.8 * dst_own))
    rounded = self_weight.astype(jnp.bfloat16).astype(jnp.float32)
    feats = own.shape[1]
    acc_ref[0, :, :feats] = rounded * own.astype(jnp.float32)
    acc_ref[0, :, feats:] = self_weight
    peak_ref[0] = jnp.max(
        jnp.maximum(jnp.abs(src_own), jnp.abs(dst_own)).reshape(rows // 8, 8, feats), axis=0
    )


def prep(own_proj, dst_table, src_exp, dst_exp, heads):
    num_blocks, rows, feats = own_proj.shape
    whole = lambda b: (0, 0, 0)
    return pl.pallas_call(
        prep_kernel,
        grid=(num_blocks,),
        in_specs=[
            pl.BlockSpec((1, rows, feats), lambda b: (b, 0, 0)),
            pl.BlockSpec(dst_table.shape, whole),
            pl.BlockSpec(src_exp.shape, whole),
            pl.BlockSpec(dst_exp.shape, whole),
        ],
        out_specs=[
            pl.BlockSpec((1, heads, rows, rows), lambda b: (b, 0, 0, 0)),
            pl.BlockSpec((1, rows, 2 * feats), lambda b: (b, 0, 0)),
            pl.BlockSpec((1, 8, feats), lambda b: (b, 0, 0)),
        ],
        out_shape=[
            jax.ShapeDtypeStruct((num_blocks, heads, rows, rows), jnp.bfloat16),
            jax.ShapeDtypeStruct((num_blocks, rows, 2 * feats), jnp.float32),
            jax.ShapeDtypeStruct((num_blocks, 8, feats), jnp.float32),
        ],
        cost_estimate=pl.CostEstimate(flops=2 * 10**9, bytes_accessed=4 * 10**6, transcendentals=10**6),
        name="prep",
    )(own_proj, dst_table, src_exp, dst_exp)


def attend_kernel(
    dst_ref,
    src_ref,
    count_ref,
    mask_ref,
    far_ref,
    ratio_ref,
    init_ref,
    peak_ref,
    att_ref,
    heads_ref,
    bias_ref,
    own_ref,
    dst_table_ref,
    src_exp_ref,
    dst_exp_ref,
    mask_hbm,
    out_ref,
    acc_ref,
    top_ref,
    slow_dst,
    slow_peak,
    slow_mask,
    slow_sem,
):
    step = pl.program_id(0)
    steps = pl.num_programs(0)
    group = mask_ref.shape[1]
    num_blocks, heads, rows, _ = ratio_ref.shape
    feats = far_ref.shape[2]
    live = count_ref[0]

    @pl.when(step == 0)
    def _():
        acc_ref[...] = init_ref[...]
        top_ref[...] = jnp.max(peak_ref[...], axis=0)

    def source_scores(values):
        parts = dot_nt(att_ref[...], values)
        return parts[0:heads] + parts[heads : 2 * heads] + parts[2 * heads : 3 * heads]

    def add_tile(block, values, weights):
        right = [
            jnp.concatenate(
                [
                    values * heads_ref[head : head + 1, :],
                    jnp.broadcast_to(heads_ref[head : head + 1, :], (rows, feats)),
                ],
                axis=1,
            )
            for head in range(heads)
        ]
        acc_ref[block] += dot_f32(jnp.concatenate(weights, axis=1), jnp.concatenate(right, axis=0))

    def fast_tile(slot, carry):
        tile = step * group + slot
        block = dst_ref[tile]
        values = far_ref[src_ref[tile]]
        scores = source_scores(values)
        top_ref[...] = jnp.maximum(top_ref[...], jnp.abs(scores))
        up = jnp.exp(scores).astype(jnp.bfloat16)
        down = jnp.exp(0.2 * scores).astype(jnp.bfloat16)
        keep = mask_ref[0, slot].astype(jnp.float32).astype(jnp.bfloat16)
        weights = []
        for head in range(heads):
            low = ratio_ref[block, head] * down[head : head + 1, :]
            weights.append(jnp.maximum(up[head : head + 1, :], low) * keep)
        add_tile(block, values, weights)
        return carry

    lax.fori_loop(0, jnp.clip(live - step * group, 0, group), fast_tile, 0)

    @pl.when(step == steps - 1)
    def _():
        in_range = jnp.max(top_ref[...]) <= LIMIT

        @pl.when(jnp.logical_not(in_range))
        def _():
            def set_block(block, carry):
                own = own_ref[block]
                wide = (
                    dot_f32(own, dst_table_ref[0])
                    + dot_f32(own, dst_table_ref[1])
                    + dot_f32(own, dst_table_ref[2])
                )
                src_own = dot_f32(own, src_exp_ref[0]) + dot_f32(own, src_exp_ref[1]) + dot_f32(own, src_exp_ref[2])
                for head in range(heads):
                    slow_dst[block, head] = wide[:, head * rows : (head + 1) * rows]
                    first = head * (feats // heads)
                    slow_peak[block, head] = jnp.broadcast_to(src_own[:, first : first + 1], (rows, rows))
                return carry

            lax.fori_loop(0, num_blocks, set_block, 0)

            def load_mask(tile):
                copy = pltpu.make_async_copy(mask_hbm.at[0, tile], slow_mask, slow_sem)
                copy.start()
                copy.wait()

            def peak_tile(tile, carry):
                load_mask(tile)
                block = dst_ref[tile]
                scores = source_scores(far_ref[src_ref[tile]])
                keep = slow_mask[...] > 0
                for head in range(heads):
                    kept = jnp.where(keep, jnp.broadcast_to(scores[head : head + 1, :], (rows, rows)), -jnp.inf)
                    tile_top = jnp.max(kept, axis=1, keepdims=True)
                    slow_peak[block, head] = jnp.maximum(slow_peak[block, head], tile_top)
                return carry

            lax.fori_loop(0, live, peak_tile, 0)

            def self_block(block, carry):
                own = own_ref[block]
                src_own = dot_f32(own, src_exp_ref[0]) + dot_f32(own, src_exp_ref[1]) + dot_f32(own, src_exp_ref[2])
                dst_own = dot_f32(own, dst_exp_ref[0]) + dot_f32(own, dst_exp_ref[1]) + dot_f32(own, dst_exp_ref[2])
                lane_head = lax.broadcasted_iota(jnp.int32, (rows, feats), 1) // (feats // heads)
                top = jnp.zeros((rows, feats), jnp.float32)
                for head in range(heads):
                    peak = leaky_relu(slow_dst[block, head] + slow_peak[block, head])
                    slow_peak[block, head] = peak
                    top = jnp.where(lane_head == head, peak, top)
                self_weight = jnp.exp(leaky_relu(dst_own + src_own) - top)
                rounded = self_weight.astype(jnp.bfloat16).astype(jnp.float32)
                acc_ref[block, :, :feats] = rounded * own.astype(jnp.float32)
                acc_ref[block, :, feats:] = self_weight
                return carry

            lax.fori_loop(0, num_blocks, self_block, 0)

            def slow_tile(tile, carry):
                load_mask(tile)
                block = dst_ref[tile]
                values = far_ref[src_ref[tile]]
                scores = source_scores(values)
                keep = slow_mask[...] > 0
                weights = []
                for head in range(heads):
                    logit = leaky_relu(slow_dst[block, head] + scores[head : head + 1, :])
                    shifted = jnp.where(keep, logit - slow_peak[block, head], -jnp.inf)
                    weights.append(jnp.exp(shifted).astype(jnp.bfloat16))
                add_tile(block, values, weights)
                return carry

            lax.fori_loop(0, live, slow_tile, 0)

        for block in range(num_blocks):
            mixed = acc_ref[block, :, :feats] / acc_ref[block, :, feats:] + bias_ref[...]
            out_ref[block] = elu(mixed).astype(out_ref.dtype)


def attend(scalars, masks, far_proj, ratio, init, peak, att3, head_rows, bias, own_proj, tables):
    _, tiles, rows, _ = masks.shape
    peers, _, feats = far_proj.shape
    num_blocks, heads = ratio.shape[:2]
    vmem = lambda: pl.BlockSpec(memory_space=pltpu.VMEM)

    def mask_map(g, dst, src, count):
        return (0, jnp.minimum(g, (count[0] - 1) // GROUP), 0, 0)

    return pl.pallas_call(
        attend_kernel,
        grid_spec=pltpu.PrefetchScalarGridSpec(
            num_scalar_prefetch=3,
            grid=(tiles // GROUP,),
            in_specs=[pl.BlockSpec((1, GROUP, rows, rows), mask_map)]
            + [vmem() for _ in range(11)]
            + [pl.BlockSpec(memory_space=pl.ANY)],
            out_specs=pl.BlockSpec((num_blocks, rows, feats), lambda g, *_: (0, 0, 0)),
            scratch_shapes=[
                pltpu.VMEM((num_blocks, rows, 2 * feats), jnp.float32),
                pltpu.VMEM((8, feats), jnp.float32),
                pltpu.VMEM((num_blocks, heads, rows, rows), jnp.float32),
                pltpu.VMEM((num_blocks, heads, rows, rows), jnp.float32),
                pltpu.VMEM((rows, rows), jnp.int32),
                pltpu.SemaphoreType.DMA,
            ],
        ),
        out_shape=jax.ShapeDtypeStruct((num_blocks, rows, feats), jnp.bfloat16),
        compiler_params=pltpu.CompilerParams(vmem_limit_bytes=60 * 1024 * 1024),
        cost_estimate=pl.CostEstimate(flops=8 * 10**9, bytes_accessed=16 * 10**6, transcendentals=10**6),
        name="attend",
    )(*scalars, masks, far_proj, ratio, init, peak, att3, head_rows, bias, own_proj, *tables, masks)


def local(
    node_feats,
    weight,
    att_src,
    att_dst,
    out_bias,
    requests,
    tile_dst,
    tile_src,
    tile_masks,
    tile_count,
):
    peers = lax.axis_size("node")
    heads, width = att_src.shape
    feats = heads * width
    rows = tile_masks.shape[2]
    num_blocks = node_feats.shape[0] // rows

    asked = jnp.broadcast_to(requests.reshape(peers, 1), (peers, feats))
    wanted = lax.all_to_all(asked, "node", split_axis=0, concat_axis=0, tiled=True)
    own_proj = jnp.dot(node_feats, weight, preferred_element_type=jnp.float32).astype(jnp.bfloat16)
    own_proj = own_proj.reshape(num_blocks, rows, feats)
    sent = gather_blocks(wanted, own_proj)
    far_proj = lax.all_to_all(sent, "node", split_axis=0, concat_axis=0, tiled=True)

    head_of = jnp.arange(feats) // width
    head_rows = (jnp.arange(heads)[:, None] == head_of[None, :])
    same_head = head_of[:, None] == head_of[None, :]
    flat_src = att_src.reshape(feats)
    flat_dst = att_dst.reshape(feats)
    att3 = jnp.concatenate(split3(jnp.where(head_rows, flat_src[None, :], 0.0)), axis=0)
    wide_head = jnp.arange(heads * rows) // rows
    dst_table = jnp.stack(split3(jnp.where(head_of[:, None] == wide_head[None, :], flat_dst[:, None], 0.0)))
    src_exp = jnp.stack(split3(jnp.where(same_head, flat_src[:, None], 0.0)))
    dst_exp = jnp.stack(split3(jnp.where(same_head, flat_dst[:, None], 0.0)))
    tables = (dst_table, src_exp, dst_exp)
    ratio, init, peak = prep(own_proj, *tables, heads)
    out = attend(
        (tile_dst.reshape(-1), tile_src.reshape(-1), tile_count),
        tile_masks,
        far_proj,
        ratio,
        init,
        peak,
        att3,
        head_rows.astype(jnp.bfloat16),
        out_bias.reshape(1, feats),
        own_proj,
        tables,
    )
    return out.reshape(num_blocks * rows, feats)


def solution(mesh):
    placed = (
        P("node", None),
        P(),
        P(),
        P(),
        P(),
        P("node", None),
        P("node", None),
        P("node", None),
        P("node", None, None, None),
        P("node"),
    )
    return jax.shard_map(
        local, mesh=mesh, in_specs=placed, out_specs=P("node", None), check_vma=False
    )
```

```python
import jax
import jax.numpy as jnp
from jax import lax
from jax.experimental import pallas as pl
from jax.experimental.pallas import tpu as pltpu
from jax.sharding import PartitionSpec as P

LIMIT = 40.0
GROUP = 16
PACK = 16
SCORE_UNROLL = 8
TILE_UNROLL = 4


def split3(table):
    high = lax.reduce_precision(table, 8, 7)
    rest = table - high
    mid = lax.reduce_precision(rest, 8, 7)
    low = rest - mid
    return tuple(part.astype(jnp.bfloat16) for part in (high, mid, low))


def leaky_relu(in_value):
    return jnp.where(in_value > 0, in_value, 0.2 * in_value)


def elu(in_value):
    return jnp.where(in_value > 0, in_value, jnp.exp(jnp.minimum(in_value, 0.0)) - 1.0)


def dot_f32(left, right):
    return jnp.dot(left, right, preferred_element_type=jnp.float32)


def dot_nt(left, right):
    return lax.dot_general(left, right, (((1,), (1,)), ((), ())), preferred_element_type=jnp.float32)


def gather_kernel(wanted_ref, own_ref, out_ref, sem):
    peers = out_ref.shape[0]

    def send(index, carry):
        for offset in range(8):
            slot = index * 8 + offset
            pltpu.make_async_copy(own_ref.at[wanted_ref[slot, 0]], out_ref.at[slot], sem).start()
        return carry

    lax.fori_loop(0, peers // 8, send, 0)
    pltpu.make_async_copy(out_ref, out_ref, sem).wait()


def gather_blocks(wanted, own_proj):
    peers, lanes = wanted.shape
    num_blocks, rows, feats = own_proj.shape
    return pl.pallas_call(
        gather_kernel,
        in_specs=[
            pl.BlockSpec(memory_space=pltpu.SMEM),
            pl.BlockSpec(memory_space=pltpu.VMEM),
        ],
        out_specs=pl.BlockSpec(memory_space=pl.ANY),
        out_shape=jax.ShapeDtypeStruct((peers, rows, feats), own_proj.dtype),
        scratch_shapes=[pltpu.SemaphoreType.DMA],
        name="gather_blocks",
    )(wanted, own_proj)


def prep_kernel(own_ref, dst_table_ref, src_exp_ref, dst_exp_ref, ratio_ref, acc_ref, peak_ref):
    own = own_ref[0]
    heads = ratio_ref.shape[1]
    rows = own.shape[0]
    dst_wide = dot_f32(own, dst_table_ref[0]) + dot_f32(own, dst_table_ref[1]) + dot_f32(own, dst_table_ref[2])
    ratio = jnp.exp(-0.8 * dst_wide).astype(jnp.bfloat16)
    for head in range(heads):
        ratio_ref[0, head] = ratio[:, head * rows : (head + 1) * rows]
    src_own = dot_f32(own, src_exp_ref[0]) + dot_f32(own, src_exp_ref[1]) + dot_f32(own, src_exp_ref[2])
    dst_own = dot_f32(own, dst_exp_ref[0]) + dot_f32(own, dst_exp_ref[1]) + dot_f32(own, dst_exp_ref[2])
    self_weight = jnp.maximum(jnp.exp(src_own), jnp.exp(0.2 * src_own - 0.8 * dst_own))
    rounded = self_weight.astype(jnp.bfloat16).astype(jnp.float32)
    feats = own.shape[1]
    acc_ref[0, :, :feats] = rounded * own.astype(jnp.float32)
    acc_ref[0, :, feats:] = self_weight
    peak_ref[0] = jnp.max(
        jnp.maximum(jnp.abs(src_own), jnp.abs(dst_own)).reshape(rows // 8, 8, feats), axis=0
    )


def prep(own_proj, dst_table, src_exp, dst_exp, heads):
    num_blocks, rows, feats = own_proj.shape
    whole = lambda b: (0, 0, 0)
    return pl.pallas_call(
        prep_kernel,
        grid=(num_blocks,),
        in_specs=[
            pl.BlockSpec((1, rows, feats), lambda b: (b, 0, 0)),
            pl.BlockSpec(dst_table.shape, whole),
            pl.BlockSpec(src_exp.shape, whole),
            pl.BlockSpec(dst_exp.shape, whole),
        ],
        out_specs=[
            pl.BlockSpec((1, heads, rows, rows), lambda b: (b, 0, 0, 0)),
            pl.BlockSpec((1, rows, 2 * feats), lambda b: (b, 0, 0)),
            pl.BlockSpec((1, 8, feats), lambda b: (b, 0, 0)),
        ],
        out_shape=[
            jax.ShapeDtypeStruct((num_blocks, heads, rows, rows), jnp.bfloat16),
            jax.ShapeDtypeStruct((num_blocks, rows, 2 * feats), jnp.float32),
            jax.ShapeDtypeStruct((num_blocks, 8, feats), jnp.float32),
        ],
        cost_estimate=pl.CostEstimate(flops=2 * 10**9, bytes_accessed=4 * 10**6, transcendentals=10**6),
        name="prep",
    )(own_proj, dst_table, src_exp, dst_exp)


def attend_kernel(
    dst_ref,
    src_ref,
    count_ref,
    mask_ref,
    far_ref,
    ratio_ref,
    init_ref,
    peak_ref,
    att_ref,
    heads_ref,
    bias_ref,
    own_ref,
    dst_table_ref,
    src_exp_ref,
    dst_exp_ref,
    mask_hbm,
    out_ref,
    acc_ref,
    top_ref,
    line_ref,
    values_ref,
    rate_ref,
    slow_dst,
    slow_peak,
    slow_mask,
    slow_sem,
):
    step = pl.program_id(0)
    steps = pl.num_programs(0)
    group = mask_ref.shape[1]
    num_blocks, heads, rows, _ = ratio_ref.shape
    feats = far_ref.shape[2]
    live = count_ref[0]

    @pl.when(step == 0)
    def _():
        acc_ref[...] = init_ref[...]
        for block in range(num_blocks):
            rate_ref[block] = ratio_ref[block]
        top_ref[...] = jnp.max(peak_ref[...], axis=0)

    def source_scores(values):
        parts = dot_nt(att_ref[...], values)
        return parts[0:heads] + parts[heads : 2 * heads] + parts[2 * heads : 3 * heads]

    def add_tile(block, values, weights):
        right = [
            jnp.concatenate(
                [
                    values * jnp.concatenate([heads_ref[head]] * (rows // PACK), axis=0),
                    jnp.concatenate([heads_ref[head]] * (rows // PACK), axis=0),
                ],
                axis=1,
            )
            for head in range(heads)
        ]
        acc_ref[block] += dot_f32(jnp.concatenate(weights, axis=1), jnp.concatenate(right, axis=0))

    def weight_rows(peer):
        block_values = far_ref[peer]
        values_ref[peer] = block_values
        scores = source_scores(block_values)
        rows_of = []
        for values in (jnp.exp(scores), jnp.exp(0.2 * scores)):
            for head in range(heads):
                wide = jnp.broadcast_to(values[head : head + 1, :], (PACK, feats))
                rows_of.append(wide.astype(jnp.bfloat16))
        return jnp.abs(scores), rows_of

    @pl.when(step == 0)
    def _():
        def score_step(index, top):
            made = [weight_rows(index * SCORE_UNROLL + offset) for offset in range(SCORE_UNROLL)]
            for offset, (size, rows_of) in enumerate(made):
                top = jnp.maximum(top, size)
                for slot in range(2 * heads):
                    line_ref[index * SCORE_UNROLL + offset, slot] = rows_of[slot]
            return top

        top_ref[...] = lax.fori_loop(0, far_ref.shape[0] // SCORE_UNROLL, score_step, top_ref[...])

    def tile_sum(slot):
        tile = step * group + slot
        block = dst_ref[tile]
        peer = src_ref[tile]
        values = values_ref[peer]
        keep = jnp.where(tile < live, mask_ref[0, slot], 0).astype(jnp.float32).astype(jnp.bfloat16)
        repeats = rows // PACK
        left, right = [], []
        for head in range(heads):
            up = jnp.concatenate([line_ref[peer, head]] * repeats, axis=0)
            down = jnp.concatenate([line_ref[peer, heads + head]] * repeats, axis=0)
            pick = jnp.concatenate([heads_ref[head]] * repeats, axis=0)
            left.append(jnp.maximum(up, rate_ref[block, head] * down) * keep)
            right.append(jnp.concatenate([values * pick, pick], axis=1))
        return block, dot_f32(jnp.concatenate(left, axis=1), jnp.concatenate(right, axis=0))

    def fast_tiles(index, carry):
        sums = [tile_sum(index * TILE_UNROLL + offset) for offset in range(TILE_UNROLL)]
        for block, total in sums:
            acc_ref[block] += total
        return carry

    here = jnp.clip(live - step * group, 0, group)
    lax.fori_loop(0, (here + TILE_UNROLL - 1) // TILE_UNROLL, fast_tiles, 0)

    @pl.when(step == steps - 1)
    def _():
        in_range = jnp.max(top_ref[...]) <= LIMIT

        @pl.when(jnp.logical_not(in_range))
        def _():
            def set_block(block, carry):
                own = own_ref[block]
                wide = (
                    dot_f32(own, dst_table_ref[0])
                    + dot_f32(own, dst_table_ref[1])
                    + dot_f32(own, dst_table_ref[2])
                )
                src_own = dot_f32(own, src_exp_ref[0]) + dot_f32(own, src_exp_ref[1]) + dot_f32(own, src_exp_ref[2])
                for head in range(heads):
                    slow_dst[block, head] = wide[:, head * rows : (head + 1) * rows]
                    first = head * (feats // heads)
                    slow_peak[block, head] = jnp.broadcast_to(src_own[:, first : first + 1], (rows, rows))
                return carry

            lax.fori_loop(0, num_blocks, set_block, 0)

            def load_mask(tile):
                copy = pltpu.make_async_copy(mask_hbm.at[0, tile], slow_mask, slow_sem)
                copy.start()
                copy.wait()

            def peak_tile(tile, carry):
                load_mask(tile)
                block = dst_ref[tile]
                scores = source_scores(far_ref[src_ref[tile]])
                keep = slow_mask[...] > 0
                for head in range(heads):
                    kept = jnp.where(keep, jnp.broadcast_to(scores[head : head + 1, :], (rows, rows)), -jnp.inf)
                    tile_top = jnp.max(kept, axis=1, keepdims=True)
                    slow_peak[block, head] = jnp.maximum(slow_peak[block, head], tile_top)
                return carry

            lax.fori_loop(0, live, peak_tile, 0)

            def self_block(block, carry):
                own = own_ref[block]
                src_own = dot_f32(own, src_exp_ref[0]) + dot_f32(own, src_exp_ref[1]) + dot_f32(own, src_exp_ref[2])
                dst_own = dot_f32(own, dst_exp_ref[0]) + dot_f32(own, dst_exp_ref[1]) + dot_f32(own, dst_exp_ref[2])
                lane_head = lax.broadcasted_iota(jnp.int32, (rows, feats), 1) // (feats // heads)
                top = jnp.zeros((rows, feats), jnp.float32)
                for head in range(heads):
                    peak = leaky_relu(slow_dst[block, head] + slow_peak[block, head])
                    slow_peak[block, head] = peak
                    top = jnp.where(lane_head == head, peak, top)
                self_weight = jnp.exp(leaky_relu(dst_own + src_own) - top)
                rounded = self_weight.astype(jnp.bfloat16).astype(jnp.float32)
                acc_ref[block, :, :feats] = rounded * own.astype(jnp.float32)
                acc_ref[block, :, feats:] = self_weight
                return carry

            lax.fori_loop(0, num_blocks, self_block, 0)

            def slow_tile(tile, carry):
                load_mask(tile)
                block = dst_ref[tile]
                values = far_ref[src_ref[tile]]
                scores = source_scores(values)
                keep = slow_mask[...] > 0
                weights = []
                for head in range(heads):
                    logit = leaky_relu(slow_dst[block, head] + scores[head : head + 1, :])
                    shifted = jnp.where(keep, logit - slow_peak[block, head], -jnp.inf)
                    weights.append(jnp.exp(shifted).astype(jnp.bfloat16))
                add_tile(block, values, weights)
                return carry

            lax.fori_loop(0, live, slow_tile, 0)

        for block in range(num_blocks):
            mixed = acc_ref[block, :, :feats] / acc_ref[block, :, feats:] + bias_ref[...]
            out_ref[block] = elu(mixed).astype(out_ref.dtype)


def attend(scalars, masks, far_proj, ratio, init, peak, att3, head_rows, bias, own_proj, tables):
    _, tiles, rows, _ = masks.shape
    peers, _, feats = far_proj.shape
    num_blocks, heads = ratio.shape[:2]
    vmem = lambda: pl.BlockSpec(memory_space=pltpu.VMEM)

    def mask_map(g, dst, src, count):
        return (0, jnp.minimum(g, (count[0] - 1) // GROUP), 0, 0)

    return pl.pallas_call(
        attend_kernel,
        grid_spec=pltpu.PrefetchScalarGridSpec(
            num_scalar_prefetch=3,
            grid=(tiles // GROUP,),
            in_specs=[pl.BlockSpec((1, GROUP, rows, rows), mask_map)]
            + [vmem() for _ in range(11)]
            + [pl.BlockSpec(memory_space=pl.ANY)],
            out_specs=pl.BlockSpec((num_blocks, rows, feats), lambda g, *_: (0, 0, 0)),
            scratch_shapes=[
                pltpu.VMEM((num_blocks, rows, 2 * feats), jnp.float32),
                pltpu.VMEM((8, feats), jnp.float32),
                pltpu.VMEM((peers, 2 * heads, PACK, feats), jnp.bfloat16),
                pltpu.VMEM((peers, rows, feats), jnp.bfloat16),
                pltpu.VMEM((num_blocks, heads, rows, rows), jnp.bfloat16),
                pltpu.VMEM((num_blocks, heads, rows, rows), jnp.float32),
                pltpu.VMEM((num_blocks, heads, rows, rows), jnp.float32),
                pltpu.VMEM((rows, rows), jnp.int32),
                pltpu.SemaphoreType.DMA,
            ],
        ),
        out_shape=jax.ShapeDtypeStruct((num_blocks, rows, feats), jnp.bfloat16),
        compiler_params=pltpu.CompilerParams(vmem_limit_bytes=60 * 1024 * 1024),
        cost_estimate=pl.CostEstimate(flops=8 * 10**9, bytes_accessed=16 * 10**6, transcendentals=10**6),
        name="attend",
    )(*scalars, masks, far_proj, ratio, init, peak, att3, head_rows, bias, own_proj, *tables, masks)


def local(
    node_feats,
    weight,
    att_src,
    att_dst,
    out_bias,
    requests,
    tile_dst,
    tile_src,
    tile_masks,
    tile_count,
):
    peers = lax.axis_size("node")
    heads, width = att_src.shape
    feats = heads * width
    rows = tile_masks.shape[2]
    num_blocks = node_feats.shape[0] // rows

    asked = jnp.broadcast_to(requests.reshape(peers, 1), (peers, feats))
    wanted = lax.all_to_all(asked, "node", split_axis=0, concat_axis=0, tiled=True)
    own_proj = jnp.dot(node_feats, weight, preferred_element_type=jnp.float32).astype(jnp.bfloat16)
    own_proj = own_proj.reshape(num_blocks, rows, feats)
    sent = gather_blocks(wanted, own_proj)
    far_proj = lax.all_to_all(sent, "node", split_axis=0, concat_axis=0, tiled=True)

    head_of = jnp.arange(feats) // width
    head_rows = (jnp.arange(heads)[:, None] == head_of[None, :])
    same_head = head_of[:, None] == head_of[None, :]
    flat_src = att_src.reshape(feats)
    flat_dst = att_dst.reshape(feats)
    att3 = jnp.concatenate(split3(jnp.where(head_rows, flat_src[None, :], 0.0)), axis=0)
    wide_head = jnp.arange(heads * rows) // rows
    dst_table = jnp.stack(split3(jnp.where(head_of[:, None] == wide_head[None, :], flat_dst[:, None], 0.0)))
    src_exp = jnp.stack(split3(jnp.where(same_head, flat_src[:, None], 0.0)))
    dst_exp = jnp.stack(split3(jnp.where(same_head, flat_dst[:, None], 0.0)))
    tables = (dst_table, src_exp, dst_exp)
    ratio, init, peak = prep(own_proj, *tables, heads)
    out = attend(
        (tile_dst.reshape(-1), tile_src.reshape(-1), tile_count),
        tile_masks,
        far_proj,
        ratio,
        init,
        peak,
        att3,
        jnp.broadcast_to(head_rows[:, None, :], (heads, PACK, feats)).astype(jnp.bfloat16),
        out_bias.reshape(1, feats),
        own_proj,
        tables,
    )
    return out.reshape(num_blocks * rows, feats)


def solution(mesh):
    placed = (
        P("node", None),
        P(),
        P(),
        P(),
        P(),
        P("node", None),
        P("node", None),
        P("node", None),
        P("node", None, None, None),
        P("node"),
    )
    return jax.shard_map(
        local, mesh=mesh, in_specs=placed, out_specs=P("node", None), check_vma=False
    )
```

```python
import functools

import jax
import jax.numpy as jnp
from jax import lax
from jax.experimental import pallas as pl
from jax.experimental.pallas import tpu as pltpu
from jax.sharding import PartitionSpec as P

LIMIT = 40.0
PACK = 16
STAGE = 8
SCORE_UNROLL = 8
TILE_UNROLL = 4
SIDE = 4
BLOCKS = 8
STRIDE = (32, 8, 2)
SHIFT = (5, 3, 1)
ROTATION = ((2, 0, 1), (0, 1, 2))
GROUPS = (((0, 0), (0, 1)), ((2, 0), (2, 1)), ((1, 0), (3, 0)), ((1, 1), (3, 1)))


def split3(table):
    high = table.astype(jnp.bfloat16)
    rest = table - high.astype(jnp.float32)
    mid = rest.astype(jnp.bfloat16)
    low = (rest - mid.astype(jnp.float32)).astype(jnp.bfloat16)
    return high, mid, low


def head_table(att):
    heads, width = att.shape
    tiled = jnp.concatenate([att] * heads, axis=1)
    lane_head = lax.broadcasted_iota(jnp.int32, tiled.shape, 1) // width
    return jnp.where(lane_head == lax.broadcasted_iota(jnp.int32, tiled.shape, 0), tiled, 0.0)


def wide_scores(values, table, repeat):
    heads, feats = table.shape
    spread_rows = jnp.concatenate(
        [jnp.broadcast_to(table[head : head + 1], (repeat, feats)) for head in range(heads)], axis=0
    )
    high, mid, low = split3(spread_rows)
    return dot_nt(values, high) + dot_nt(values, mid) + dot_nt(values, low)


def leaky_relu(in_value):
    return jnp.where(in_value > 0, in_value, 0.2 * in_value)


def elu(in_value):
    return jnp.where(in_value > 0, in_value, jnp.exp(jnp.minimum(in_value, 0.0)) - 1.0)


def dot_f32(left, right):
    return jnp.dot(left, right, preferred_element_type=jnp.float32)


def dot_nt(left, right):
    return lax.dot_general(left, right, (((1,), (1,)), ((), ())), preferred_element_type=jnp.float32)


def project_kernel(weight_ref, *refs):
    pieces, out_ref = refs[:-1], refs[-1]
    _, rows, feats = out_ref.shape
    for piece in range(len(pieces)):
        made = dot_f32(pieces[piece][...], weight_ref[...]).astype(out_ref.dtype)
        out_ref[piece * BLOCKS : (piece + 1) * BLOCKS] = made.reshape(BLOCKS, rows, feats)


def project(pieces, weight):
    rows = pieces[0].shape[0] // BLOCKS
    feats = weight.shape[1]
    return pl.pallas_call(
        project_kernel,
        out_shape=jax.ShapeDtypeStruct((len(pieces) * BLOCKS, rows, feats), jnp.bfloat16),
        cost_estimate=pl.CostEstimate(flops=2 * 10**9, bytes_accessed=2 * 10**6, transcendentals=0),
compiler_params=pltpu.CompilerParams(vmem_limit_bytes=8 * 1024 * 1024),
        name="project",
    )(weight, *pieces)


def by_core(core, pair):
    return jnp.where(core == 0, pair[0], pair[1])


def place_of(device):
    core = device & 1
    place = [(device >> shift) & (SIDE - 1) for shift in SHIFT]
    here = [by_core(core, [place[ROTATION[owner][phase]] for owner in range(2)]) for phase in range(3)]
    step = [by_core(core, [STRIDE[ROTATION[owner][phase]] for owner in range(2)]) for phase in range(3)]
    return core, place, here, step


def pick_kernel(device_ref, lines_ref, *refs):
    pieces, outs = refs[:SIDE], refs[SIDE:]
    core, _, here, step = place_of(device_ref[0])
    for second in range(SIDE):
        for first in range(SIDE):
            peer = (
                ((here[0] - first) & (SIDE - 1)) * step[0]
                + ((here[1] - second) & (SIDE - 1)) * step[1]
                + here[2] * step[2]
                + core
            )
            for hop in range(SIDE):
                for half in range(2):
                    chosen = lines_ref[(SIDE - hop) % SIDE * 2 + half, peer]
                    outs[hop * 2 + half][second * SIDE + first] = pieces[second][first * BLOCKS + chosen]


def pick_blocks(device, lines, pieces):
    rows, feats = pieces[0].shape[1:]
    return pl.pallas_call(
        pick_kernel,
        in_specs=[pl.BlockSpec(memory_space=pltpu.SMEM)] * 2
        + [pl.BlockSpec(memory_space=pltpu.VMEM)] * SIDE,
        out_specs=[pl.BlockSpec(memory_space=pltpu.VMEM)] * (2 * SIDE),
        out_shape=[jax.ShapeDtypeStruct((SIDE * SIDE, rows, feats), jnp.bfloat16)] * (2 * SIDE),
        compiler_params=pltpu.CompilerParams(vmem_limit_bytes=12 * 1024 * 1024),
        cost_estimate=pl.CostEstimate(flops=2 * 10**8, bytes_accessed=4 * 10**6, transcendentals=0),
        name="pick_blocks",
    )(device, lines, *pieces)


def route(axes, shift, swap=0):
    pairs = []
    for device in range(2 * SIDE**3):
        stride = STRIDE[axes[device % 2]]
        place = device // stride % SIDE
        target = device + ((place + shift) % SIDE - place) * stride
        pairs.append((device, target ^ swap))
    return pairs


def shift_along(value, phase, shift, swap=0):
    axes = tuple(ROTATION[core][phase] for core in range(2))
    return lax.ppermute(value, "node", route(axes, shift, swap))


def spread(value, phase):
    moved = {hop: shift_along(value, phase, hop) for hop in (2, 1, 3)}
    return [value] + [moved[hop] for hop in range(1, SIDE)]


def ready_kernel(device_ref, dst_ref, src_ref, count_ref, mask_hbm, list_ref, spot_ref, out_ref, stage_ref, sems):
    tiles = src_ref.shape[0]
    live = count_ref[0]
    rounds = (live + STAGE - 1) // STAGE

    def stage_copy(index):
        source = mask_hbm.at[0, pl.ds(index * STAGE, STAGE)]
        return pltpu.make_async_copy(source, stage_ref.at[index & 3], sems.at[index & 3])

    for index in range(3):

        @pl.when(index < rounds)
        def _():
            stage_copy(index).start()

    core, place, _, _ = place_of(device_ref[0])

    def place_tile(tile, counts):
        peer = src_ref[tile]
        away = [(place[axis] - (peer >> SHIFT[axis])) & (SIDE - 1) for axis in range(3)]
        first, second, third = [
            by_core(peer & 1, [away[ROTATION[owner][phase]] for owner in range(2)]) for phase in range(3)
        ]
        half = (peer & 1) ^ core
        even = (third & 1) == 0
        group = jnp.where(even, third >> 1, 2 + half)
        local_spot = (jnp.where(even, half, third >> 1) * SIDE + second) * SIDE + first
        spot_ref[tile] = group * 2 * SIDE * SIDE + local_spot
        at = sum(jnp.where(group == part, counts[part], 0) for part in range(len(GROUPS)))
        list_ref[group * 3, at] = tile
        list_ref[group * 3 + 1, at] = dst_ref[tile]
        list_ref[group * 3 + 2, at] = local_spot
        return tuple(counts[part] + jnp.where(group == part, 1, 0) for part in range(len(GROUPS)))

    counts = lax.fori_loop(0, live, place_tile, (jnp.int32(0),) * len(GROUPS))
    for part in range(len(GROUPS)):
        list_ref[3 * len(GROUPS), part] = counts[part]
        for extra in range(TILE_UNROLL - 1):
            list_ref[part * 3, counts[part] + extra] = tiles
            list_ref[part * 3 + 1, counts[part] + extra] = 0
            list_ref[part * 3 + 2, counts[part] + extra] = 0
    out_ref[tiles] = jnp.zeros(out_ref.shape[1:], jnp.float32)

    def stage_round(index, carry):
        @pl.when(index + 3 < rounds)
        def _():
            stage_copy(index + 3).start()

        stage_copy(index).wait()
        for offset in range(STAGE):
            out_ref[index * STAGE + offset] = stage_ref[index & 3, offset].astype(jnp.float32)
        return carry

    lax.fori_loop(0, rounds, stage_round, 0)


def ready(device, tile_dst, tile_src, tile_count, masks):
    _, tiles, rows, _ = masks.shape
    smem = pl.BlockSpec(memory_space=pltpu.SMEM)
    return pl.pallas_call(
        ready_kernel,
        in_specs=[smem] * 4 + [pl.BlockSpec(memory_space=pl.ANY)],
        out_specs=[smem, smem, pl.BlockSpec(memory_space=pltpu.VMEM)],
        out_shape=[
            jax.ShapeDtypeStruct((3 * len(GROUPS) + 1, tiles + TILE_UNROLL), jnp.int32),
            jax.ShapeDtypeStruct((tiles,), jnp.int32),
            jax.ShapeDtypeStruct((tiles + 1, rows, rows), jnp.float32),
        ],
        scratch_shapes=[pltpu.VMEM((4, STAGE, rows, rows), jnp.int32), pltpu.SemaphoreType.DMA((4,))],
        compiler_params=pltpu.CompilerParams(vmem_limit_bytes=48 * 1024 * 1024),
        cost_estimate=pl.CostEstimate(flops=3 * 10**9, bytes_accessed=12 * 10**6, transcendentals=0),
        name="ready",
    )(device, tile_dst, tile_src, tile_count, masks)


def prep_kernel(own_ref, att_src_ref, att_dst_ref, ratio_ref, acc_ref, peak_ref, att_ref, heads_ref):
    own = own_ref[0]
    heads = ratio_ref.shape[1]
    rows = own.shape[0]
    src_table = head_table(att_src_ref[...])
    dst_table = head_table(att_dst_ref[...])
    att_ref[...] = jnp.concatenate([part.astype(jnp.float32) for part in split3(src_table)], axis=0)
    lane_head = lax.broadcasted_iota(jnp.int32, (8, own.shape[1]), 1) // att_src_ref.shape[1]
    for head in range(heads):
        heads_ref[head] = jnp.where(lane_head == head, 1.0, 0.0)
    ratio = jnp.exp(-0.8 * wide_scores(own, dst_table, rows))
    for head in range(heads):
        ratio_ref[0, head] = ratio[:, head * rows : (head + 1) * rows]
    src_own = wide_scores(own, src_table, att_src_ref.shape[1])
    dst_own = wide_scores(own, dst_table, att_src_ref.shape[1])
    self_weight = jnp.maximum(jnp.exp(src_own), jnp.exp(0.2 * src_own - 0.8 * dst_own))
    rounded = self_weight.astype(jnp.bfloat16).astype(jnp.float32)
    feats = own.shape[1]
    acc_ref[0, :, :feats] = rounded * own.astype(jnp.float32)
    acc_ref[0, :, feats:] = self_weight
    size = jnp.maximum(jnp.abs(src_own), jnp.abs(dst_own)).reshape(rows // 8, 8, feats)

    @pl.when(pl.program_id(0) == 0)
    def _():
        peak_ref[...] = jnp.zeros_like(peak_ref)

    peak_ref[...] = jnp.maximum(peak_ref[...], jnp.max(size, axis=0))


def prep(own_proj, att_src, att_dst):
    _, rows, feats = own_proj.shape
    heads = att_src.shape[0]
    whole = lambda b: (0, 0)
    return pl.pallas_call(
        prep_kernel,
        grid=(BLOCKS,),
        in_specs=[
            pl.BlockSpec((1, rows, feats), lambda b: (b, 0, 0)),
            pl.BlockSpec(att_src.shape, whole),
            pl.BlockSpec(att_dst.shape, whole),
        ],
        out_specs=[
            pl.BlockSpec((1, heads, rows, rows), lambda b: (b, 0, 0, 0)),
            pl.BlockSpec((1, rows, 2 * feats), lambda b: (b, 0, 0)),
            pl.BlockSpec((8, feats), whole),
            pl.BlockSpec((3 * heads, feats), whole),
            pl.BlockSpec((heads, 8, feats), lambda b: (0, 0, 0)),
        ],
        out_shape=[
            jax.ShapeDtypeStruct((BLOCKS, heads, rows, rows), jnp.float32),
            jax.ShapeDtypeStruct((BLOCKS, rows, 2 * feats), jnp.float32),
            jax.ShapeDtypeStruct((8, feats), jnp.float32),
            jax.ShapeDtypeStruct((3 * heads, feats), jnp.float32),
            jax.ShapeDtypeStruct((heads, 8, feats), jnp.float32),
        ],
        compiler_params=pltpu.CompilerParams(vmem_limit_bytes=16 * 1024 * 1024),
        cost_estimate=pl.CostEstimate(flops=3 * 10**9, bytes_accessed=4 * 10**6, transcendentals=10**6),
        name="prep",
    )(own_proj, att_src, att_dst)


def source_scores(att_ref, values, heads):
    parts = dot_nt(att_ref[...].astype(jnp.bfloat16), values)
    return parts[0:heads] + parts[heads : 2 * heads] + parts[2 * heads : 3 * heads]


def wide_row(row, rows):
    pair = jnp.concatenate([row] * (PACK // row.shape[0]), axis=0).astype(jnp.bfloat16)
    return jnp.concatenate([pair] * (rows // PACK), axis=0)


def tile_product(left, values, heads_ref):
    rows = values.shape[0]
    right = []
    for head in range(len(left)):
        pick = wide_row(heads_ref[head], rows)
        right.append(jnp.concatenate([values * pick, pick], axis=1))
    return dot_f32(jnp.concatenate(left, axis=1), jnp.concatenate(right, axis=0))


def half_pass(part, list_ref, masks_ref, pieces, ratio_ref, att_ref, heads_ref, acc_ref, top_ref, line_ref, values_ref):
    _, heads, rows, _ = ratio_ref.shape
    feats = values_ref.shape[2]
    size = SIDE * SIDE
    rounds = (list_ref[3 * len(GROUPS), part] + TILE_UNROLL - 1) // TILE_UNROLL

    def weight_rows(piece, slot, from_slot):
        block_values = piece[from_slot]
        values_ref[slot] = block_values.astype(jnp.float32)
        scores = source_scores(att_ref, block_values, heads)
        made = []
        for values in (jnp.exp(scores), jnp.exp(0.2 * scores)):
            for head in range(heads):
                made.append(jnp.broadcast_to(values[head : head + 1, :], (8, feats)))
        return jnp.abs(scores), made

    top = top_ref[...]
    for number, piece in enumerate(pieces):

        def score_step(index, top):
            first = index * SCORE_UNROLL
            all_made = [
                weight_rows(piece, number * size + first + offset, first + offset) for offset in range(SCORE_UNROLL)
            ]
            for offset, (extent, made) in enumerate(all_made):
                top = jnp.maximum(top, extent)
                for row in range(2 * heads):
                    line_ref[number * size + first + offset, row] = made[row]
            return top

        top = lax.fori_loop(0, size // SCORE_UNROLL, score_step, top)
    top_ref[...] = top

    def tile_sum(place):
        block = list_ref[part * 3 + 1, place]
        spot = list_ref[part * 3 + 2, place]
        keep = masks_ref[list_ref[part * 3, place]].astype(jnp.bfloat16)
        left = []
        for head in range(heads):
            up = wide_row(line_ref[spot, head], rows)
            down = wide_row(line_ref[spot, heads + head], rows)
            left.append(jnp.maximum(up, ratio_ref[block, head].astype(jnp.bfloat16) * down) * keep)
        return block, tile_product(left, values_ref[spot].astype(jnp.bfloat16), heads_ref)

    def tile_round(index, carry):
        first = index * TILE_UNROLL
        sums = [tile_sum(first + offset) for offset in range(TILE_UNROLL)]
        for block, total in sums:
            acc_ref[block] += total
        return carry

    lax.fori_loop(0, rounds, tile_round, 0)


def step_kernel(part, list_ref, masks_ref, ratio_ref, init_ref, peak_ref, att_ref, heads_ref, *refs):
    pieces, (acc_ref, top_ref), scratch = refs[:-4], refs[-4:-2], refs[-2:]
    half_pass(part, list_ref, masks_ref, pieces, ratio_ref, att_ref, heads_ref, acc_ref, top_ref, *scratch)


def half_scratch(rows, feats, heads, pieces):
    slots = len(pieces) * pieces[0].shape[0]
    return [
        pltpu.VMEM((slots, 2 * heads, 8, feats), jnp.float32),
        pltpu.VMEM((slots, rows, feats), jnp.float32),
    ]


def attend_step(part, tile_rows, masks, ratio, acc, top, att3, head_rows, pieces):
    num_blocks, heads, rows, _ = ratio.shape
    feats = att3.shape[1]
    return pl.pallas_call(
        functools.partial(step_kernel, part),
        in_specs=[pl.BlockSpec(memory_space=pltpu.SMEM)]
        + [pl.BlockSpec(memory_space=pltpu.VMEM)] * (6 + len(pieces)),
        out_specs=[pl.BlockSpec(memory_space=pltpu.VMEM)] * 2,
        out_shape=[
            jax.ShapeDtypeStruct((num_blocks, rows, 2 * feats), jnp.float32),
            jax.ShapeDtypeStruct((8, feats), jnp.float32),
        ],
        scratch_shapes=half_scratch(rows, feats, heads, pieces),
        compiler_params=pltpu.CompilerParams(vmem_limit_bytes=10 * 1024 * 1024),
        cost_estimate=pl.CostEstimate(flops=6 * 10**9, bytes_accessed=8 * 10**6, transcendentals=10**6),
        input_output_aliases={3: 0, 4: 1},
        name="attend_step",
    )(tile_rows, masks, ratio, acc, top, att3, head_rows, *pieces)


def finish_kernel(
    acc_ref,
    top_ref,
    bias_ref,
    dst_ref,
    spot_ref,
    count_ref,
    att_ref,
    heads_ref,
    att_src_ref,
    att_dst_ref,
    mask_hbm,
    own_hbm,
    *refs,
):
    pieces, out_ref = refs[:-7], refs[-7]
    own_ref, far_ref, slow_dst, slow_peak, slow_mask, slow_sem = refs[-6:]
    num_blocks, rows, feats = out_ref.shape
    heads = heads_ref.shape[0]
    in_range = jnp.max(top_ref[...]) <= LIMIT

    def finish(block, sums):
        mixed = sums[:, :feats] / sums[:, feats:] + bias_ref[...]
        out_ref[block] = elu(mixed).astype(out_ref.dtype)

    for block in range(num_blocks):
        finish(block, acc_ref[block])

    @pl.when(jnp.logical_not(in_range))
    def _():
        live = count_ref[0]

        def load(source, target):
            copy = pltpu.make_async_copy(source, target, slow_sem)
            copy.start()
            copy.wait()

        load(own_hbm.at[pl.ds(0, num_blocks)], own_ref)
        src_table = head_table(att_src_ref[...])
        dst_table = head_table(att_dst_ref[...])
        width = att_src_ref.shape[1]
        part = SIDE * SIDE
        for index, piece in enumerate(pieces):
            load(piece, far_ref.at[pl.ds(index * part, part)])

        def set_block(block, carry):
            own = own_ref[block]
            wide = wide_scores(own, dst_table, rows)
            src_own = wide_scores(own, src_table, width)
            for head in range(heads):
                slow_dst[block, head] = wide[:, head * rows : (head + 1) * rows]
                first = head * (feats // heads)
                slow_peak[block, head] = jnp.broadcast_to(src_own[:, first : first + 1], (rows, rows))
            return carry

        lax.fori_loop(0, num_blocks, set_block, 0)

        def peak_tile(tile, carry):
            block = dst_ref[tile]
            scores = source_scores(att_ref, far_ref[spot_ref[tile]], heads)
            load(mask_hbm.at[0, tile], slow_mask)
            keep = slow_mask[...] > 0
            for head in range(heads):
                kept = jnp.where(keep, jnp.broadcast_to(scores[head : head + 1, :], (rows, rows)), -jnp.inf)
                tile_top = jnp.max(kept, axis=1, keepdims=True)
                slow_peak[block, head] = jnp.maximum(slow_peak[block, head], tile_top)
            return carry

        lax.fori_loop(0, live, peak_tile, 0)

        def self_block(block, carry):
            own = own_ref[block]
            src_own = wide_scores(own, src_table, width)
            dst_own = wide_scores(own, dst_table, width)
            lane_head = lax.broadcasted_iota(jnp.int32, (rows, feats), 1) // (feats // heads)
            top = jnp.zeros((rows, feats), jnp.float32)
            for head in range(heads):
                peak = leaky_relu(slow_dst[block, head] + slow_peak[block, head])
                slow_peak[block, head] = peak
                top = jnp.where(lane_head == head, peak, top)
            self_weight = jnp.exp(leaky_relu(dst_own + src_own) - top)
            rounded = self_weight.astype(jnp.bfloat16).astype(jnp.float32)
            acc_ref[block, :, :feats] = rounded * own.astype(jnp.float32)
            acc_ref[block, :, feats:] = self_weight
            return carry

        lax.fori_loop(0, num_blocks, self_block, 0)

        def slow_tile(tile, carry):
            block = dst_ref[tile]
            values = far_ref[spot_ref[tile]]
            scores = source_scores(att_ref, values, heads)
            load(mask_hbm.at[0, tile], slow_mask)
            keep = slow_mask[...] > 0
            left = []
            for head in range(heads):
                logit = leaky_relu(slow_dst[block, head] + scores[head : head + 1, :])
                shifted = jnp.where(keep, logit - slow_peak[block, head], -jnp.inf)
                left.append(jnp.exp(shifted).astype(jnp.bfloat16))
            acc_ref[block] += tile_product(left, values, heads_ref)
            return carry

        lax.fori_loop(0, live, slow_tile, 0)
        for block in range(num_blocks):
            finish(block, acc_ref[block])


def finish_all(acc, top, bias, scalars, att3, head_rows, atts, masks, own_proj, pieces):
    num_blocks, rows, double = acc.shape
    feats = double // 2
    heads = head_rows.shape[0]
    vmem = pl.BlockSpec(memory_space=pltpu.VMEM)
    return pl.pallas_call(
        finish_kernel,
        in_specs=[vmem] * 3
        + [pl.BlockSpec(memory_space=pltpu.SMEM)] * 3
        + [vmem] * 4
        + [pl.BlockSpec(memory_space=pl.ANY)] * (2 + len(pieces)),
        out_specs=vmem,
        out_shape=jax.ShapeDtypeStruct((num_blocks, rows, feats), jnp.bfloat16),
        scratch_shapes=[
            pltpu.VMEM((num_blocks, rows, feats), jnp.bfloat16),
            pltpu.VMEM((2 * SIDE**3, rows, feats), jnp.bfloat16),
            pltpu.VMEM((num_blocks, heads, rows, rows), jnp.float32),
            pltpu.VMEM((num_blocks, heads, rows, rows), jnp.float32),
            pltpu.VMEM((rows, rows), jnp.int32),
            pltpu.SemaphoreType.DMA,
        ],
        compiler_params=pltpu.CompilerParams(vmem_limit_bytes=16 * 1024 * 1024),
        cost_estimate=pl.CostEstimate(flops=10**9, bytes_accessed=2 * 10**6, transcendentals=10**6),
        name="finish",
    )(acc, top, bias, *scalars, att3, head_rows, *atts, masks, own_proj, *pieces)


def local(
    node_feats,
    weight,
    att_src,
    att_dst,
    out_bias,
    requests,
    tile_dst,
    tile_src,
    tile_masks,
    tile_count,
):
    feats = att_src.size
    rows = tile_masks.shape[2]
    num_blocks = node_feats.shape[0] // rows
    device = lax.axis_index("node").astype(jnp.int32).reshape(1)

    line = project(spread(node_feats, 0), weight)
    planes = spread(line, 1)

    dst_ids = tile_dst.reshape(-1)
    lists, spots, masks = ready(device, dst_ids, tile_src.reshape(-1), tile_count, tile_masks)
    pair = jnp.concatenate([requests, shift_along(requests, 0, 0, 1)], axis=0)
    lines = jnp.concatenate(spread(pair, 2), axis=0)
    ratio, init, peak, att3, picks = prep(line, att_src, att_dst)

    held = lax.optimization_barrier((planes, lines, ratio, init, peak, att3, picks, lists, spots, masks))
    planes, lines, ratio, init, peak, att3, picks, lists, spots, masks = held
    picked = pick_blocks(device, lines, planes)
    arrived = {(hop, half): picked[2 * hop + half] for hop in range(SIDE) for half in range(2)}
    arrived[0, 1] = shift_along(arrived[0, 1], 2, 0, 1)
    for hop, half in ((2, 0), (2, 1), (1, 0), (3, 0), (1, 1), (3, 1)):
        arrived[hop, half] = shift_along(arrived[hop, half], 2, hop, half)
    landed = [[arrived[key] for key in keys] for keys in GROUPS]

    acc, top = init, peak
    for part in range(len(GROUPS)):
        acc, top = attend_step(part, lists, masks, ratio, acc, top, att3, picks, landed[part])
    out = finish_all(
        acc,
        top,
        out_bias.reshape(1, feats),
        (dst_ids, spots, tile_count),
        att3,
        picks,
        (att_src, att_dst),
        tile_masks,
        line,
        sum(landed, []),
    )
    return out.reshape(num_blocks * rows, feats)


def solution(mesh):
    placed = (
        P("node", None),
        P(),
        P(),
        P(),
        P(),
        P("node", None),
        P("node", None),
        P("node", None),
        P("node", None, None, None),
        P("node"),
    )
    return jax.shard_map(
        local, mesh=mesh, in_specs=placed, out_specs=P("node", None), check_vma=False
    )
```

```python
import functools

import jax
import jax.numpy as jnp
from jax import lax
from jax.experimental import pallas as pl
from jax.experimental.pallas import tpu as pltpu
from jax.sharding import PartitionSpec as P

LIMIT = 40.0
PACK = 16
STAGE = 8
SCORE_UNROLL = 8
TILE_UNROLL = 4
SIDE = 4
BLOCKS = 8
STRIDE = (32, 8, 2)
SHIFT = (5, 3, 1)
ROTATION = ((2, 0, 1), (0, 1, 2))
GROUPS = (((0, 0), (0, 1)), ((2, 0), (2, 1)), ((1, 0), (3, 0)), ((1, 1), (3, 1)))


def split3(table):
    high = table.astype(jnp.bfloat16)
    rest = table - high.astype(jnp.float32)
    mid = rest.astype(jnp.bfloat16)
    low = (rest - mid.astype(jnp.float32)).astype(jnp.bfloat16)
    return high, mid, low


def head_table(att):
    heads, width = att.shape
    tiled = jnp.concatenate([att] * heads, axis=1)
    lane_head = lax.broadcasted_iota(jnp.int32, tiled.shape, 1) // width
    return jnp.where(lane_head == lax.broadcasted_iota(jnp.int32, tiled.shape, 0), tiled, 0.0)


def wide_scores(values, table, repeat):
    heads, feats = table.shape
    spread_rows = jnp.concatenate(
        [jnp.broadcast_to(table[head : head + 1], (repeat, feats)) for head in range(heads)], axis=0
    )
    high, mid, low = split3(spread_rows)
    return dot_nt(values, high) + dot_nt(values, mid) + dot_nt(values, low)


def leaky_relu(in_value):
    return jnp.where(in_value > 0, in_value, 0.2 * in_value)


def elu(in_value):
    return jnp.where(in_value > 0, in_value, jnp.exp(jnp.minimum(in_value, 0.0)) - 1.0)


def dot_f32(left, right):
    return jnp.dot(left, right, preferred_element_type=jnp.float32)


def dot_nt(left, right):
    return lax.dot_general(left, right, (((1,), (1,)), ((), ())), preferred_element_type=jnp.float32)


def stage_kernel(feats_ref, weight_ref, own_ref, weight_copy):
    own_ref[...] = dot_f32(feats_ref[...], weight_ref[...]).astype(own_ref.dtype)
    weight_copy[...] = weight_ref[...]


def project_own(node_feats, weight):
    return pl.pallas_call(
        stage_kernel,
        out_shape=[
            jax.ShapeDtypeStruct((node_feats.shape[0], weight.shape[1]), jnp.bfloat16),
            jax.ShapeDtypeStruct(weight.shape, weight.dtype),
        ],
        compiler_params=pltpu.CompilerParams(vmem_limit_bytes=8 * 1024 * 1024),
        cost_estimate=pl.CostEstimate(flops=10**9, bytes_accessed=10**6, transcendentals=0),
        name="project_own",
    )(node_feats, weight)


def pair_kernel(own_ref, partner_ref, out_ref):
    out_ref[0:1] = own_ref[...]
    out_ref[1:2] = partner_ref[...]


def pair_rows(own, partner):
    return pl.pallas_call(
        pair_kernel,
        out_shape=jax.ShapeDtypeStruct((2, own.shape[1]), own.dtype),
        compiler_params=pltpu.CompilerParams(vmem_limit_bytes=1024 * 1024),
        name="pair_rows",
    )(own, partner)


def project_kernel(weight_ref, own_ref, piece1, piece2, piece3, *refs):
    low_ref, high_ref = refs[-2:]
    _, rows, feats = low_ref.shape
    project_one = lambda piece: dot_f32(piece[...], weight_ref[...]).astype(low_ref.dtype)
    low_ref[:BLOCKS] = own_ref[...].reshape(BLOCKS, rows, feats)
    low_ref[BLOCKS:] = project_one(piece1).reshape(BLOCKS, rows, feats)
    high_ref[:BLOCKS] = project_one(piece2).reshape(BLOCKS, rows, feats)
    high_ref[BLOCKS:] = project_one(piece3).reshape(BLOCKS, rows, feats)


def project(own, pieces, weight, after):
    rows = own.shape[0] // BLOCKS
    feats = weight.shape[1]
    return pl.pallas_call(
        project_kernel,
        in_specs=[pl.BlockSpec(memory_space=pltpu.VMEM)] * 5 + [pl.BlockSpec(memory_space=pl.ANY)] * len(after),
        out_shape=[jax.ShapeDtypeStruct((SIDE * BLOCKS // 2, rows, feats), jnp.bfloat16)] * 2,
        compiler_params=pltpu.CompilerParams(vmem_limit_bytes=8 * 1024 * 1024),
        cost_estimate=pl.CostEstimate(flops=2 * 10**9, bytes_accessed=2 * 10**6, transcendentals=0),
        name="project",
    )(weight, own, *pieces, *after)


def by_core(core, pair):
    return jnp.where(core == 0, pair[0], pair[1])


def place_of(device):
    core = device & 1
    place = [(device >> shift) & (SIDE - 1) for shift in SHIFT]
    here = [by_core(core, [place[ROTATION[owner][phase]] for owner in range(2)]) for phase in range(3)]
    step = [by_core(core, [STRIDE[ROTATION[owner][phase]] for owner in range(2)]) for phase in range(3)]
    return core, place, here, step


def pick_kernel(device_ref, *refs):
    lines, pieces, outs = refs[:SIDE], refs[SIDE : 3 * SIDE], refs[3 * SIDE :]
    core, _, here, step = place_of(device_ref[0])
    for second in range(SIDE):
        for first in range(SIDE):
            peer = (
                ((here[0] - first) & (SIDE - 1)) * step[0]
                + ((here[1] - second) & (SIDE - 1)) * step[1]
                + here[2] * step[2]
                + core
            )
            piece = pieces[second * 2 + first // 2]
            for hop in range(SIDE):
                for half in range(2):
                    chosen = lines[(SIDE - hop) % SIDE][half, peer]
                    outs[hop * 2 + half][second * SIDE + first] = piece[first % 2 * BLOCKS + chosen]


def pick_blocks(device, lines, pieces):
    rows, feats = pieces[0].shape[1:]
    return pl.pallas_call(
        pick_kernel,
        in_specs=[pl.BlockSpec(memory_space=pltpu.SMEM)] * (1 + SIDE)
        + [pl.BlockSpec(memory_space=pltpu.VMEM)] * (2 * SIDE),
        out_specs=[pl.BlockSpec(memory_space=pltpu.VMEM)] * (2 * SIDE),
        out_shape=[jax.ShapeDtypeStruct((SIDE * SIDE, rows, feats), jnp.bfloat16)] * (2 * SIDE),
        compiler_params=pltpu.CompilerParams(vmem_limit_bytes=12 * 1024 * 1024),
        cost_estimate=pl.CostEstimate(flops=2 * 10**8, bytes_accessed=4 * 10**6, transcendentals=0),
        name="pick_blocks",
    )(device, *lines, *pieces)


def route(axes, shift, swap=0):
    pairs = []
    for device in range(2 * SIDE**3):
        stride = STRIDE[axes[device % 2]]
        place = device // stride % SIDE
        target = device + ((place + shift) % SIDE - place) * stride
        pairs.append((device, target ^ swap))
    return pairs


def shift_along(value, phase, shift, swap=0):
    axes = tuple(ROTATION[core][phase] for core in range(2))
    return lax.ppermute(value, "node", route(axes, shift, swap))


def spread(value, phase):
    moved = {hop: shift_along(value, phase, hop) for hop in (2, 1, 3)}
    return [value] + [moved[hop] for hop in range(1, SIDE)]


def ready_kernel(device_ref, count_ref, dst_ref, src_ref, list_ref, spot_ref):
    tiles = src_ref.shape[1]
    core, place, _, _ = place_of(device_ref[0])
    peer = src_ref[...]
    away = [(place[axis] - (peer >> SHIFT[axis])) & (SIDE - 1) for axis in range(3)]
    owner = peer & 1
    first, second, third = [
        jnp.where(owner == 0, away[ROTATION[0][phase]], away[ROTATION[1][phase]]) for phase in range(3)
    ]
    half = owner ^ core
    even = (third & 1) == 0
    group = jnp.where(even, third >> 1, 2 + half)
    local_spot = (jnp.where(even, half, third >> 1) * SIDE + second) * SIDE + first
    spot_ref[...] = group * 2 * SIDE * SIDE + local_spot
    tile = lax.broadcasted_iota(jnp.int32, (1, tiles), 1)
    group = jnp.where(tile < count_ref[0], group, 8)
    one = lambda hit: jnp.where(hit, 1.0, 0.0)
    member = one(lax.broadcasted_iota(jnp.int32, (8, tiles), 0) == group)
    up = lax.broadcasted_iota(jnp.int32, (tiles, tiles), 0)
    across = lax.broadcasted_iota(jnp.int32, (tiles, tiles), 1)
    before = dot_f32(member.astype(jnp.bfloat16), one(up < across).astype(jnp.bfloat16))
    rank = jnp.sum(member * before, axis=0, keepdims=True).astype(jnp.int32)
    row = lax.broadcasted_iota(jnp.int32, (8, tiles), 0)
    facts = jnp.where(row == 0, tile, jnp.where(row == 1, dst_ref[...] + 8 * local_spot, 0))
    facts = facts.astype(jnp.float32).astype(jnp.bfloat16)
    for part in range(len(GROUPS)):
        hit = (rank == up) & (group == part)
        found = dot_nt(facts, one(hit).astype(jnp.bfloat16))
        list_ref[part : part + 1] = (found[0:1] + 256.0 * found[1:2]).astype(jnp.int32)
    total = jnp.sum(member, axis=1, keepdims=True).astype(jnp.int32)
    list_ref[8:16] = jnp.broadcast_to(total, (8, tiles))


def ready(device, tile_dst, tile_src, tile_count):
    tiles = tile_src.shape[1]
    smem = pl.BlockSpec(memory_space=pltpu.SMEM)
    vmem = pl.BlockSpec(memory_space=pltpu.VMEM)
    return pl.pallas_call(
        ready_kernel,
        in_specs=[smem, smem, vmem, vmem],
        out_specs=[vmem, vmem],
        out_shape=[
            jax.ShapeDtypeStruct((16, tiles), jnp.int32),
            jax.ShapeDtypeStruct((1, tiles), jnp.int32),
        ],
        compiler_params=pltpu.CompilerParams(vmem_limit_bytes=4 * 1024 * 1024),
        cost_estimate=pl.CostEstimate(flops=10**9, bytes_accessed=10**5, transcendentals=0),
        name="ready",
    )(device, tile_count, tile_dst, tile_src)


def masks_kernel(count_ref, mask_hbm, out_ref, stage_ref, sems):
    tiles = mask_hbm.shape[1]
    rounds = (count_ref[0] + STAGE - 1) // STAGE

    def stage_copy(index):
        source = mask_hbm.at[0, pl.ds(index * STAGE, STAGE)]
        return pltpu.make_async_copy(source, stage_ref.at[index & 3], sems.at[index & 3])

    for index in range(3):

        @pl.when(index < rounds)
        def _():
            stage_copy(index).start()

    out_ref[tiles] = jnp.zeros(out_ref.shape[1:], out_ref.dtype)

    def stage_round(index, carry):
        @pl.when(index + 3 < rounds)
        def _():
            stage_copy(index + 3).start()

        stage_copy(index).wait()
        for offset in range(STAGE):
            out_ref[index * STAGE + offset] = stage_ref[index & 3, offset].astype(jnp.float32).astype(out_ref.dtype)
        return carry

    lax.fori_loop(0, rounds, stage_round, 0)


def stage_masks(tile_count, masks):
    _, tiles, rows, _ = masks.shape
    return pl.pallas_call(
        masks_kernel,
        in_specs=[pl.BlockSpec(memory_space=pltpu.SMEM), pl.BlockSpec(memory_space=pl.ANY)],
        out_specs=pl.BlockSpec(memory_space=pltpu.VMEM),
        out_shape=jax.ShapeDtypeStruct((tiles + 1, rows, rows), jnp.bfloat16),
        scratch_shapes=[pltpu.VMEM((4, STAGE, rows, rows), jnp.int32), pltpu.SemaphoreType.DMA((4,))],
        compiler_params=pltpu.CompilerParams(vmem_limit_bytes=48 * 1024 * 1024),
        cost_estimate=pl.CostEstimate(flops=3 * 10**9, bytes_accessed=12 * 10**6, transcendentals=0),
        name="stage_masks",
    )(tile_count, masks)


def prep_kernel(own_ref, att_src_ref, att_dst_ref, ratio_ref, acc_ref, peak_ref, att_ref, heads_ref):
    own = own_ref[0]
    heads = ratio_ref.shape[1]
    rows = own.shape[0]
    src_table = head_table(att_src_ref[...])
    dst_table = head_table(att_dst_ref[...])
    att_ref[...] = jnp.concatenate([part.astype(jnp.float32) for part in split3(src_table)], axis=0)
    lane_head = lax.broadcasted_iota(jnp.int32, (8, own.shape[1]), 1) // att_src_ref.shape[1]
    for head in range(heads):
        heads_ref[head] = jnp.where(lane_head == head, 1.0, 0.0)
    ratio = jnp.exp(-0.8 * wide_scores(own, dst_table, rows))
    for head in range(heads):
        ratio_ref[0, head] = ratio[:, head * rows : (head + 1) * rows]
    src_own = wide_scores(own, src_table, att_src_ref.shape[1])
    dst_own = wide_scores(own, dst_table, att_src_ref.shape[1])
    self_weight = jnp.maximum(jnp.exp(src_own), jnp.exp(0.2 * src_own - 0.8 * dst_own))
    rounded = self_weight.astype(jnp.bfloat16).astype(jnp.float32)
    feats = own.shape[1]
    acc_ref[0, :, :feats] = rounded * own.astype(jnp.float32)
    acc_ref[0, :, feats:] = self_weight
    size = jnp.maximum(jnp.abs(src_own), jnp.abs(dst_own)).reshape(rows // 8, 8, feats)

    @pl.when(pl.program_id(0) == 0)
    def _():
        peak_ref[...] = jnp.zeros_like(peak_ref)

    peak_ref[...] = jnp.maximum(peak_ref[...], jnp.max(size, axis=0))


def prep(own_proj, att_src, att_dst):
    _, rows, feats = own_proj.shape
    heads = att_src.shape[0]
    whole = lambda b: (0, 0)
    return pl.pallas_call(
        prep_kernel,
        grid=(BLOCKS,),
        in_specs=[
            pl.BlockSpec((1, rows, feats), lambda b: (b, 0, 0)),
            pl.BlockSpec(att_src.shape, whole),
            pl.BlockSpec(att_dst.shape, whole),
        ],
        out_specs=[
            pl.BlockSpec((1, heads, rows, rows), lambda b: (b, 0, 0, 0)),
            pl.BlockSpec((1, rows, 2 * feats), lambda b: (b, 0, 0)),
            pl.BlockSpec((8, feats), whole),
            pl.BlockSpec((3 * heads, feats), whole),
            pl.BlockSpec((heads, 8, feats), lambda b: (0, 0, 0)),
        ],
        out_shape=[
            jax.ShapeDtypeStruct((BLOCKS, heads, rows, rows), jnp.float32),
            jax.ShapeDtypeStruct((BLOCKS, rows, 2 * feats), jnp.float32),
            jax.ShapeDtypeStruct((8, feats), jnp.float32),
            jax.ShapeDtypeStruct((3 * heads, feats), jnp.float32),
            jax.ShapeDtypeStruct((heads, 8, feats), jnp.float32),
        ],
        compiler_params=pltpu.CompilerParams(vmem_limit_bytes=16 * 1024 * 1024),
        cost_estimate=pl.CostEstimate(flops=3 * 10**9, bytes_accessed=4 * 10**6, transcendentals=10**6),
        name="prep",
    )(own_proj, att_src, att_dst)


def source_scores(att_ref, values, heads):
    parts = dot_nt(att_ref[...].astype(jnp.bfloat16), values)
    return parts[0:heads] + parts[heads : 2 * heads] + parts[2 * heads : 3 * heads]


def wide_row(row, rows):
    pair = jnp.concatenate([row] * (PACK // row.shape[0]), axis=0).astype(jnp.bfloat16)
    return jnp.concatenate([pair] * (rows // PACK), axis=0)


def tile_product(left, values, heads_ref):
    rows = values.shape[0]
    right = []
    for head in range(len(left)):
        pick = wide_row(heads_ref[head], rows)
        right.append(jnp.concatenate([values * pick, pick], axis=1))
    return dot_f32(jnp.concatenate(left, axis=1), jnp.concatenate(right, axis=0))


def half_pass(part, list_ref, masks_ref, pieces, ratio_ref, att_ref, heads_ref, acc_ref, top_ref, line_ref, values_ref):
    _, heads, rows, _ = ratio_ref.shape
    feats = values_ref.shape[2]
    size = SIDE * SIDE
    live = list_ref[8 + part, 0]
    rounds = (live + TILE_UNROLL - 1) // TILE_UNROLL

    def weight_rows(piece, slot, from_slot):
        block_values = piece[from_slot]
        values_ref[slot] = block_values.astype(jnp.float32)
        scores = source_scores(att_ref, block_values, heads)
        made = []
        for values in (jnp.exp(scores), jnp.exp(0.2 * scores)):
            for head in range(heads):
                made.append(jnp.broadcast_to(values[head : head + 1, :], (8, feats)))
        return jnp.abs(scores), made

    top = top_ref[...]
    for number, piece in enumerate(pieces):

        def score_step(index, top):
            first = index * SCORE_UNROLL
            all_made = [
                weight_rows(piece, number * size + first + offset, first + offset) for offset in range(SCORE_UNROLL)
            ]
            for offset, (extent, made) in enumerate(all_made):
                top = jnp.maximum(top, extent)
                for row in range(2 * heads):
                    line_ref[number * size + first + offset, row] = made[row]
            return top

        top = lax.fori_loop(0, size // SCORE_UNROLL, score_step, top)
    top_ref[...] = top

    def tile_sum(place):
        entry = list_ref[part, jnp.minimum(place, list_ref.shape[1] - 1)]
        block = (entry >> 8) & (BLOCKS - 1)
        spot = entry >> 11
        keep = masks_ref[jnp.where(place < live, entry & 255, masks_ref.shape[0] - 1)]
        left = []
        for head in range(heads):
            up = wide_row(line_ref[spot, head], rows)
            down = wide_row(line_ref[spot, heads + head], rows)
            left.append(jnp.maximum(up, ratio_ref[block, head].astype(jnp.bfloat16) * down) * keep)
        return block, tile_product(left, values_ref[spot].astype(jnp.bfloat16), heads_ref)

    def tile_round(index, carry):
        first = index * TILE_UNROLL
        sums = [tile_sum(first + offset) for offset in range(TILE_UNROLL)]
        for block, total in sums:
            acc_ref[block] += total
        return carry

    lax.fori_loop(0, rounds, tile_round, 0)


def step_kernel(part, list_ref, masks_ref, ratio_ref, init_ref, peak_ref, att_ref, heads_ref, *refs):
    pieces, (acc_ref, top_ref), scratch = refs[:-4], refs[-4:-2], refs[-2:]
    half_pass(part, list_ref, masks_ref, pieces, ratio_ref, att_ref, heads_ref, acc_ref, top_ref, *scratch)


def half_scratch(rows, feats, heads, pieces):
    slots = len(pieces) * pieces[0].shape[0]
    return [
        pltpu.VMEM((slots, 2 * heads, 8, feats), jnp.float32),
        pltpu.VMEM((slots, rows, feats), jnp.float32),
    ]


def attend_step(part, tile_rows, masks, ratio, acc, top, att3, head_rows, pieces):
    num_blocks, heads, rows, _ = ratio.shape
    feats = att3.shape[1]
    return pl.pallas_call(
        functools.partial(step_kernel, part),
        in_specs=[pl.BlockSpec(memory_space=pltpu.SMEM)]
        + [pl.BlockSpec(memory_space=pltpu.VMEM)] * (6 + len(pieces)),
        out_specs=[pl.BlockSpec(memory_space=pltpu.VMEM)] * 2,
        out_shape=[
            jax.ShapeDtypeStruct((num_blocks, rows, 2 * feats), jnp.float32),
            jax.ShapeDtypeStruct((8, feats), jnp.float32),
        ],
        scratch_shapes=half_scratch(rows, feats, heads, pieces),
        compiler_params=pltpu.CompilerParams(vmem_limit_bytes=10 * 1024 * 1024),
        cost_estimate=pl.CostEstimate(flops=6 * 10**9, bytes_accessed=8 * 10**6, transcendentals=10**6),
        input_output_aliases={3: 0, 4: 1},
        name="attend_step",
    )(tile_rows, masks, ratio, acc, top, att3, head_rows, *pieces)


def last_kernel(
    part,
    list_ref,
    masks_ref,
    ratio_ref,
    init_ref,
    peak_ref,
    att_ref,
    heads_ref,
    bias_ref,
    dst_ref,
    spot_ref,
    count_ref,
    att_src_ref,
    att_dst_ref,
    own_hbm,
    *refs,
):
    early, pieces, out_ref = refs[:-12], refs[-12:-10], refs[-10]
    acc_ref, top_ref, line_ref, values_ref, own_ref, far_ref, slow_dst, slow_peak, slow_sem = refs[-9:]
    acc_ref[...] = init_ref[...]
    top_ref[...] = peak_ref[...]
    half_pass(part, list_ref, masks_ref, pieces, ratio_ref, att_ref, heads_ref, acc_ref, top_ref, line_ref, values_ref)
    num_blocks, rows, feats = out_ref.shape
    heads = heads_ref.shape[0]
    in_range = jnp.max(top_ref[...]) <= LIMIT

    def finish(block, sums):
        mixed = sums[:, :feats] / sums[:, feats:] + bias_ref[...]
        out_ref[block] = elu(mixed).astype(out_ref.dtype)

    for block in range(num_blocks):
        finish(block, acc_ref[block])

    @pl.when(jnp.logical_not(in_range))
    def _():
        live = count_ref[0]

        def load(source, target):
            copy = pltpu.make_async_copy(source, target, slow_sem)
            copy.start()
            copy.wait()

        load(own_hbm.at[pl.ds(0, num_blocks)], own_ref)
        src_table = head_table(att_src_ref[...])
        dst_table = head_table(att_dst_ref[...])
        width = att_src_ref.shape[1]
        size = SIDE * SIDE
        for index, piece in enumerate(early + pieces):
            load(piece, far_ref.at[pl.ds(index * size, size)])

        def set_block(block, carry):
            own = own_ref[block]
            wide = wide_scores(own, dst_table, rows)
            src_own = wide_scores(own, src_table, width)
            for head in range(heads):
                slow_dst[block, head] = wide[:, head * rows : (head + 1) * rows]
                first = head * (feats // heads)
                slow_peak[block, head] = jnp.broadcast_to(src_own[:, first : first + 1], (rows, rows))
            return carry

        lax.fori_loop(0, num_blocks, set_block, 0)

        def peak_tile(tile, carry):
            block = dst_ref[0, tile]
            scores = source_scores(att_ref, far_ref[spot_ref[0, tile]], heads)
            keep = masks_ref[tile].astype(jnp.float32) > 0
            for head in range(heads):
                kept = jnp.where(keep, jnp.broadcast_to(scores[head : head + 1, :], (rows, rows)), -jnp.inf)
                tile_top = jnp.max(kept, axis=1, keepdims=True)
                slow_peak[block, head] = jnp.maximum(slow_peak[block, head], tile_top)
            return carry

        lax.fori_loop(0, live, peak_tile, 0)

        def self_block(block, carry):
            own = own_ref[block]
            src_own = wide_scores(own, src_table, width)
            dst_own = wide_scores(own, dst_table, width)
            lane_head = lax.broadcasted_iota(jnp.int32, (rows, feats), 1) // (feats // heads)
            top = jnp.zeros((rows, feats), jnp.float32)
            for head in range(heads):
                peak = leaky_relu(slow_dst[block, head] + slow_peak[block, head])
                slow_peak[block, head] = peak
                top = jnp.where(lane_head == head, peak, top)
            self_weight = jnp.exp(leaky_relu(dst_own + src_own) - top)
            rounded = self_weight.astype(jnp.bfloat16).astype(jnp.float32)
            acc_ref[block, :, :feats] = rounded * own.astype(jnp.float32)
            acc_ref[block, :, feats:] = self_weight
            return carry

        lax.fori_loop(0, num_blocks, self_block, 0)

        def slow_tile(tile, carry):
            block = dst_ref[0, tile]
            values = far_ref[spot_ref[0, tile]]
            scores = source_scores(att_ref, values, heads)
            keep = masks_ref[tile].astype(jnp.float32) > 0
            left = []
            for head in range(heads):
                logit = leaky_relu(slow_dst[block, head] + scores[head : head + 1, :])
                shifted = jnp.where(keep, logit - slow_peak[block, head], -jnp.inf)
                left.append(jnp.exp(shifted).astype(jnp.bfloat16))
            acc_ref[block] += tile_product(left, values, heads_ref)
            return carry

        lax.fori_loop(0, live, slow_tile, 0)
        for block in range(num_blocks):
            finish(block, acc_ref[block])


def attend_last(lists, masks, ratio, acc, top, att3, head_rows, bias, scalars, atts, own_proj, early, pieces):
    num_blocks, heads, rows, _ = ratio.shape
    feats = att3.shape[1]
    vmem = pl.BlockSpec(memory_space=pltpu.VMEM)
    smem = pl.BlockSpec(memory_space=pltpu.SMEM)
    return pl.pallas_call(
        functools.partial(last_kernel, len(GROUPS) - 1),
        in_specs=[smem]
        + [vmem] * 7
        + [smem] * 3
        + [vmem] * 2
        + [pl.BlockSpec(memory_space=pl.ANY)] * (1 + len(early))
        + [vmem] * len(pieces),
        out_specs=vmem,
        out_shape=jax.ShapeDtypeStruct((num_blocks, rows, feats), jnp.bfloat16),
        scratch_shapes=[pltpu.VMEM(acc.shape, acc.dtype), pltpu.VMEM(top.shape, top.dtype)]
        + half_scratch(rows, feats, heads, pieces)
        + [
            pltpu.VMEM((num_blocks, rows, feats), jnp.bfloat16),
            pltpu.VMEM((2 * SIDE**3, rows, feats), jnp.bfloat16),
            pltpu.VMEM((num_blocks, heads, rows, rows), jnp.float32),
            pltpu.VMEM((num_blocks, heads, rows, rows), jnp.float32),
            pltpu.SemaphoreType.DMA,
        ],
        compiler_params=pltpu.CompilerParams(vmem_limit_bytes=20 * 1024 * 1024),
        cost_estimate=pl.CostEstimate(flops=7 * 10**9, bytes_accessed=8 * 10**6, transcendentals=10**6),
        name="attend_last",
    )(lists, masks, ratio, acc, top, att3, head_rows, bias, *scalars, *atts, own_proj, *early, *pieces)


def local(
    node_feats,
    weight,
    att_src,
    att_dst,
    out_bias,
    requests,
    tile_dst,
    tile_src,
    tile_masks,
    tile_count,
):
    feats = att_src.size
    rows = tile_masks.shape[2]
    num_blocks = node_feats.shape[0] // rows
    device = lax.axis_index("node").astype(jnp.int32).reshape(1)

    pair = pair_rows(requests, shift_along(requests, 0, 0, 1))
    lines = spread(pair, 2)
    own, staged = project_own(node_feats, weight)
    low, high = project(own, spread(node_feats, 0)[1:], staged, lines[1:])
    left_low = shift_along(low, 1, 1)
    right_high = shift_along(high, 1, 3)
    left_high = shift_along(high, 1, 1)
    right_low = shift_along(low, 1, 3)
    far_low = shift_along(left_low, 1, 1)
    far_high = shift_along(right_high, 1, 3)
    planes = [low, high, left_low, left_high, far_low, far_high, right_low, right_high]
    own_blocks = own.reshape(num_blocks, rows, feats)

    masks = stage_masks(tile_count, tile_masks)
    lists, spots = ready(device, tile_dst, tile_src, tile_count)
    ratio, init, peak, att3, picks = prep(own_blocks, att_src, att_dst)

    held = lax.optimization_barrier((planes, lines, ratio, init, peak, att3, picks, lists, spots, masks))
    planes, lines, ratio, init, peak, att3, picks, lists, spots, masks = held
    picked = pick_blocks(device, lines, planes)
    arrived = {(hop, half): picked[2 * hop + half] for hop in range(SIDE) for half in range(2)}
    arrived[0, 1] = shift_along(arrived[0, 1], 2, 0, 1)
    for hop, half in ((2, 0), (2, 1), (1, 0), (3, 0), (1, 1), (3, 1)):
        arrived[hop, half] = shift_along(arrived[hop, half], 2, hop, half)
    landed = [[arrived[key] for key in keys] for keys in GROUPS]

    acc, top = init, peak
    for part in range(len(GROUPS) - 1):
        acc, top = attend_step(part, lists, masks, ratio, acc, top, att3, picks, landed[part])
    out = attend_last(
        lists,
        masks,
        ratio,
        acc,
        top,
        att3,
        picks,
        out_bias.reshape(1, feats),
        (tile_dst, spots, tile_count),
        (att_src, att_dst),
        own_blocks,
        sum(landed[:-1], []),
        landed[-1],
    )
    return out.reshape(num_blocks * rows, feats)


def solution(mesh):
    placed = (
        P("node", None),
        P(),
        P(),
        P(),
        P(),
        P("node", None),
        P("node", None),
        P("node", None),
        P("node", None, None, None),
        P("node"),
    )
    return jax.shard_map(
        local, mesh=mesh, in_specs=placed, out_specs=P("node", None), check_vma=False
    )
```

```python
import functools

import jax
import jax.numpy as jnp
from jax import lax
from jax.experimental import pallas as pl
from jax.experimental.pallas import tpu as pltpu
from jax.sharding import PartitionSpec as P

LIMIT = 40.0
PACK = 16
STAGE = 8
SCORE_UNROLL = 16
TILE_UNROLL = 8
SIDE = 4
BLOCKS = 8
STRIDE = (32, 8, 2)
SHIFT = (5, 3, 1)
ROTATION = ((2, 0, 1), (0, 1, 2))
GROUPS = (((0, 0), (0, 1)), ((2, 0), (2, 1)), ((1, 0), (3, 0)), ((1, 1), (3, 1)))


def split3(table):
    high = table.astype(jnp.bfloat16)
    rest = table - high.astype(jnp.float32)
    mid = rest.astype(jnp.bfloat16)
    low = (rest - mid.astype(jnp.float32)).astype(jnp.bfloat16)
    return high, mid, low


def head_table(att):
    heads, width = att.shape
    tiled = jnp.concatenate([att] * heads, axis=1)
    lane_head = lax.broadcasted_iota(jnp.int32, tiled.shape, 1) // width
    return jnp.where(lane_head == lax.broadcasted_iota(jnp.int32, tiled.shape, 0), tiled, 0.0)


def wide_scores(values, table, repeat):
    heads, feats = table.shape
    spread_rows = jnp.concatenate(
        [jnp.broadcast_to(table[head : head + 1], (repeat, feats)) for head in range(heads)], axis=0
    )
    high, mid, low = split3(spread_rows)
    return dot_nt(values, high) + dot_nt(values, mid) + dot_nt(values, low)


def leaky_relu(in_value):
    return jnp.where(in_value > 0, in_value, 0.2 * in_value)


def elu(in_value):
    return jnp.where(in_value > 0, in_value, jnp.exp(jnp.minimum(in_value, 0.0)) - 1.0)


def dot_f32(left, right):
    return jnp.dot(left, right, preferred_element_type=jnp.float32)


def dot_nt(left, right):
    return lax.dot_general(left, right, (((1,), (1,)), ((), ())), preferred_element_type=jnp.float32)


def stage_kernel(feats_ref, weight_ref, own_ref, weight_copy):
    own_ref[...] = dot_f32(feats_ref[...], weight_ref[...]).astype(own_ref.dtype)
    weight_copy[...] = weight_ref[...]


def project_own(node_feats, weight):
    return pl.pallas_call(
        stage_kernel,
        out_shape=[
            jax.ShapeDtypeStruct((node_feats.shape[0], weight.shape[1]), jnp.bfloat16),
            jax.ShapeDtypeStruct(weight.shape, weight.dtype),
        ],
        compiler_params=pltpu.CompilerParams(vmem_limit_bytes=8 * 1024 * 1024),
        cost_estimate=pl.CostEstimate(flops=10**9, bytes_accessed=10**6, transcendentals=0),
        name="project_own",
    )(node_feats, weight)


def pair_kernel(own_ref, partner_ref, out_ref):
    out_ref[0:1] = own_ref[...]
    out_ref[1:2] = partner_ref[...]


def pair_rows(own, partner):
    return pl.pallas_call(
        pair_kernel,
        out_shape=jax.ShapeDtypeStruct((2, own.shape[1]), own.dtype),
        compiler_params=pltpu.CompilerParams(vmem_limit_bytes=1024 * 1024),
        name="pair_rows",
    )(own, partner)


def project_kernel(weight_ref, own_ref, piece1, piece2, piece3, *refs):
    low_ref, high_ref = refs[-2:]
    _, rows, feats = low_ref.shape
    project_one = lambda piece: dot_f32(piece[...], weight_ref[...]).astype(low_ref.dtype)
    low_ref[:BLOCKS] = own_ref[...].reshape(BLOCKS, rows, feats)
    low_ref[BLOCKS:] = project_one(piece1).reshape(BLOCKS, rows, feats)
    high_ref[:BLOCKS] = project_one(piece2).reshape(BLOCKS, rows, feats)
    high_ref[BLOCKS:] = project_one(piece3).reshape(BLOCKS, rows, feats)


def project(own, pieces, weight, after):
    rows = own.shape[0] // BLOCKS
    feats = weight.shape[1]
    return pl.pallas_call(
        project_kernel,
        in_specs=[pl.BlockSpec(memory_space=pltpu.VMEM)] * 5 + [pl.BlockSpec(memory_space=pl.ANY)] * len(after),
        out_shape=[jax.ShapeDtypeStruct((SIDE * BLOCKS // 2, rows, feats), jnp.bfloat16)] * 2,
        compiler_params=pltpu.CompilerParams(vmem_limit_bytes=8 * 1024 * 1024),
        cost_estimate=pl.CostEstimate(flops=2 * 10**9, bytes_accessed=2 * 10**6, transcendentals=0),
        name="project",
    )(weight, own, *pieces, *after)


def by_core(core, pair):
    return jnp.where(core == 0, pair[0], pair[1])


def place_of(device):
    core = device & 1
    place = [(device >> shift) & (SIDE - 1) for shift in SHIFT]
    here = [by_core(core, [place[ROTATION[owner][phase]] for owner in range(2)]) for phase in range(3)]
    step = [by_core(core, [STRIDE[ROTATION[owner][phase]] for owner in range(2)]) for phase in range(3)]
    return core, place, here, step


def pick_kernel(device_ref, *refs):
    lines, pieces, outs = refs[:SIDE], refs[SIDE : 3 * SIDE], refs[3 * SIDE :]
    core, _, here, step = place_of(device_ref[0])
    for second in range(SIDE):
        for first in range(SIDE):
            peer = (
                ((here[0] - first) & (SIDE - 1)) * step[0]
                + ((here[1] - second) & (SIDE - 1)) * step[1]
                + here[2] * step[2]
                + core
            )
            piece = pieces[second * 2 + first // 2]
            for hop in range(SIDE):
                for half in range(2):
                    chosen = lines[(SIDE - hop) % SIDE][half, peer]
                    outs[hop * 2 + half][second * SIDE + first] = piece[first % 2 * BLOCKS + chosen]


def pick_blocks(device, lines, pieces):
    rows, feats = pieces[0].shape[1:]
    return pl.pallas_call(
        pick_kernel,
        in_specs=[pl.BlockSpec(memory_space=pltpu.SMEM)] * (1 + SIDE)
        + [pl.BlockSpec(memory_space=pltpu.VMEM)] * (2 * SIDE),
        out_specs=[pl.BlockSpec(memory_space=pltpu.VMEM)] * (2 * SIDE),
        out_shape=[jax.ShapeDtypeStruct((SIDE * SIDE, rows, feats), jnp.bfloat16)] * (2 * SIDE),
        compiler_params=pltpu.CompilerParams(vmem_limit_bytes=12 * 1024 * 1024),
        cost_estimate=pl.CostEstimate(flops=2 * 10**8, bytes_accessed=4 * 10**6, transcendentals=0),
        name="pick_blocks",
    )(device, *lines, *pieces)


def route(axes, shift, swap=0):
    pairs = []
    for device in range(2 * SIDE**3):
        stride = STRIDE[axes[device % 2]]
        place = device // stride % SIDE
        target = device + ((place + shift) % SIDE - place) * stride
        pairs.append((device, target ^ swap))
    return pairs


def shift_along(value, phase, shift, swap=0):
    axes = tuple(ROTATION[core][phase] for core in range(2))
    return lax.ppermute(value, "node", route(axes, shift, swap))


def spread(value, phase):
    moved = {hop: shift_along(value, phase, hop) for hop in (2, 1, 3)}
    return [value] + [moved[hop] for hop in range(1, SIDE)]


def ready_kernel(device_ref, count_ref, dst_ref, src_ref, list_ref, spot_ref):
    tiles = src_ref.shape[1]
    core, place, _, _ = place_of(device_ref[0])
    peer = src_ref[...]
    away = [(place[axis] - (peer >> SHIFT[axis])) & (SIDE - 1) for axis in range(3)]
    owner = peer & 1
    first, second, third = [
        jnp.where(owner == 0, away[ROTATION[0][phase]], away[ROTATION[1][phase]]) for phase in range(3)
    ]
    half = owner ^ core
    even = (third & 1) == 0
    group = jnp.where(even, third >> 1, 2 + half)
    local_spot = (jnp.where(even, half, third >> 1) * SIDE + second) * SIDE + first
    spot_ref[...] = group * 2 * SIDE * SIDE + local_spot
    tile = lax.broadcasted_iota(jnp.int32, (1, tiles), 1)
    group = jnp.where(tile < count_ref[0], group, 8)
    one = lambda hit: jnp.where(hit, 1.0, 0.0)
    member = one(lax.broadcasted_iota(jnp.int32, (8, tiles), 0) == group)
    up = lax.broadcasted_iota(jnp.int32, (tiles, tiles), 0)
    across = lax.broadcasted_iota(jnp.int32, (tiles, tiles), 1)
    before = dot_f32(member.astype(jnp.bfloat16), one(up < across).astype(jnp.bfloat16))
    rank = jnp.sum(member * before, axis=0, keepdims=True).astype(jnp.int32)
    row = lax.broadcasted_iota(jnp.int32, (8, tiles), 0)
    facts = jnp.where(row == 0, tile, jnp.where(row == 1, dst_ref[...] + 8 * local_spot, 0))
    facts = facts.astype(jnp.float32).astype(jnp.bfloat16)
    for part in range(len(GROUPS)):
        hit = (rank == up) & (group == part)
        found = dot_nt(facts, one(hit).astype(jnp.bfloat16))
        list_ref[part : part + 1] = (found[0:1] + 256.0 * found[1:2]).astype(jnp.int32)
    total = jnp.sum(member, axis=1, keepdims=True).astype(jnp.int32)
    list_ref[8:16] = jnp.broadcast_to(total, (8, tiles))


def ready(device, tile_dst, tile_src, tile_count):
    tiles = tile_src.shape[1]
    smem = pl.BlockSpec(memory_space=pltpu.SMEM)
    vmem = pl.BlockSpec(memory_space=pltpu.VMEM)
    return pl.pallas_call(
        ready_kernel,
        in_specs=[smem, smem, vmem, vmem],
        out_specs=[vmem, vmem],
        out_shape=[
            jax.ShapeDtypeStruct((16, tiles), jnp.int32),
            jax.ShapeDtypeStruct((1, tiles), jnp.int32),
        ],
        compiler_params=pltpu.CompilerParams(vmem_limit_bytes=4 * 1024 * 1024),
        cost_estimate=pl.CostEstimate(flops=10**9, bytes_accessed=10**5, transcendentals=0),
        name="ready",
    )(device, tile_count, tile_dst, tile_src)


def masks_kernel(count_ref, mask_hbm, out_ref, stage_ref, sems):
    tiles = mask_hbm.shape[1]
    rounds = (count_ref[0] + STAGE - 1) // STAGE

    def stage_copy(index):
        source = mask_hbm.at[0, pl.ds(index * STAGE, STAGE)]
        return pltpu.make_async_copy(source, stage_ref.at[index & 3], sems.at[index & 3])

    for index in range(3):

        @pl.when(index < rounds)
        def _():
            stage_copy(index).start()

    out_ref[tiles] = jnp.zeros(out_ref.shape[1:], out_ref.dtype)

    def stage_round(index, carry):
        @pl.when(index + 3 < rounds)
        def _():
            stage_copy(index + 3).start()

        stage_copy(index).wait()
        for offset in range(STAGE):
            out_ref[index * STAGE + offset] = stage_ref[index & 3, offset].astype(jnp.float32).astype(out_ref.dtype)
        return carry

    lax.fori_loop(0, rounds, stage_round, 0)


def stage_masks(tile_count, masks):
    _, tiles, rows, _ = masks.shape
    return pl.pallas_call(
        masks_kernel,
        in_specs=[pl.BlockSpec(memory_space=pltpu.SMEM), pl.BlockSpec(memory_space=pl.ANY)],
        out_specs=pl.BlockSpec(memory_space=pltpu.VMEM),
        out_shape=jax.ShapeDtypeStruct((tiles + 1, rows, rows), jnp.bfloat16),
        scratch_shapes=[pltpu.VMEM((4, STAGE, rows, rows), jnp.int32), pltpu.SemaphoreType.DMA((4,))],
        compiler_params=pltpu.CompilerParams(vmem_limit_bytes=48 * 1024 * 1024),
        cost_estimate=pl.CostEstimate(flops=3 * 10**9, bytes_accessed=12 * 10**6, transcendentals=0),
        name="stage_masks",
    )(tile_count, masks)


def prep_kernel(own_ref, att_src_ref, att_dst_ref, ratio_ref, acc_ref, peak_ref, att_ref, heads_ref):
    own = own_ref[0]
    heads = ratio_ref.shape[1]
    rows = own.shape[0]
    src_table = head_table(att_src_ref[...])
    dst_table = head_table(att_dst_ref[...])
    att_ref[...] = jnp.concatenate([part.astype(jnp.float32) for part in split3(src_table)], axis=0)
    lane_head = lax.broadcasted_iota(jnp.int32, (8, own.shape[1]), 1) // att_src_ref.shape[1]
    for head in range(heads):
        heads_ref[head] = jnp.where(lane_head == head, 1.0, 0.0)
    ratio = jnp.exp(-0.8 * wide_scores(own, dst_table, rows))
    for head in range(heads):
        ratio_ref[0, head] = ratio[:, head * rows : (head + 1) * rows]
    src_own = wide_scores(own, src_table, att_src_ref.shape[1])
    dst_own = wide_scores(own, dst_table, att_src_ref.shape[1])
    self_weight = jnp.maximum(jnp.exp(src_own), jnp.exp(0.2 * src_own - 0.8 * dst_own))
    rounded = self_weight.astype(jnp.bfloat16).astype(jnp.float32)
    feats = own.shape[1]
    acc_ref[0, :, :feats] = rounded * own.astype(jnp.float32)
    acc_ref[0, :, feats:] = self_weight
    size = jnp.maximum(jnp.abs(src_own), jnp.abs(dst_own)).reshape(rows // 8, 8, feats)

    @pl.when(pl.program_id(0) == 0)
    def _():
        peak_ref[...] = jnp.zeros_like(peak_ref)

    peak_ref[...] = jnp.maximum(peak_ref[...], jnp.max(size, axis=0))


def prep(own_proj, att_src, att_dst):
    _, rows, feats = own_proj.shape
    heads = att_src.shape[0]
    whole = lambda b: (0, 0)
    return pl.pallas_call(
        prep_kernel,
        grid=(BLOCKS,),
        in_specs=[
            pl.BlockSpec((1, rows, feats), lambda b: (b, 0, 0)),
            pl.BlockSpec(att_src.shape, whole),
            pl.BlockSpec(att_dst.shape, whole),
        ],
        out_specs=[
            pl.BlockSpec((1, heads, rows, rows), lambda b: (b, 0, 0, 0)),
            pl.BlockSpec((1, rows, 2 * feats), lambda b: (b, 0, 0)),
            pl.BlockSpec((8, feats), whole),
            pl.BlockSpec((3 * heads, feats), whole),
            pl.BlockSpec((heads, 8, feats), lambda b: (0, 0, 0)),
        ],
        out_shape=[
            jax.ShapeDtypeStruct((BLOCKS, heads, rows, rows), jnp.float32),
            jax.ShapeDtypeStruct((BLOCKS, rows, 2 * feats), jnp.float32),
            jax.ShapeDtypeStruct((8, feats), jnp.float32),
            jax.ShapeDtypeStruct((3 * heads, feats), jnp.float32),
            jax.ShapeDtypeStruct((heads, 8, feats), jnp.float32),
        ],
        compiler_params=pltpu.CompilerParams(vmem_limit_bytes=16 * 1024 * 1024),
        cost_estimate=pl.CostEstimate(flops=3 * 10**9, bytes_accessed=4 * 10**6, transcendentals=10**6),
        name="prep",
    )(own_proj, att_src, att_dst)


def source_scores(att_ref, values, heads):
    parts = dot_nt(att_ref[...].astype(jnp.bfloat16), values)
    return parts[0:heads] + parts[heads : 2 * heads] + parts[2 * heads : 3 * heads]


def wide_row(row, rows):
    pair = jnp.concatenate([row] * (PACK // row.shape[0]), axis=0).astype(jnp.bfloat16)
    return jnp.concatenate([pair] * (rows // PACK), axis=0)


def tile_product(left, values, heads_ref):
    rows = values.shape[0]
    right = []
    for head in range(len(left)):
        pick = wide_row(heads_ref[head], rows)
        right.append(jnp.concatenate([values * pick, pick], axis=1))
    return dot_f32(jnp.concatenate(left, axis=1), jnp.concatenate(right, axis=0))


def half_pass(part, list_ref, masks_ref, pieces, ratio_ref, att_ref, heads_ref, acc_ref, top_ref, line_ref, values_ref):
    _, heads, rows, _ = ratio_ref.shape
    feats = values_ref.shape[2]
    size = SIDE * SIDE
    live = list_ref[8 + part, 0]
    rounds = (live + TILE_UNROLL - 1) // TILE_UNROLL

    def weight_rows(piece, slot, from_slot):
        block_values = piece[from_slot]
        values_ref[slot] = block_values.astype(jnp.float32)
        scores = source_scores(att_ref, block_values, heads)
        made = []
        for values in (jnp.exp(scores), jnp.exp(0.2 * scores)):
            for head in range(heads):
                made.append(jnp.broadcast_to(values[head : head + 1, :], (8, feats)))
        return jnp.abs(scores), made

    top = top_ref[...]
    for number, piece in enumerate(pieces):

        def score_step(index, top):
            first = index * SCORE_UNROLL
            all_made = [
                weight_rows(piece, number * size + first + offset, first + offset) for offset in range(SCORE_UNROLL)
            ]
            for offset, (extent, made) in enumerate(all_made):
                top = jnp.maximum(top, extent)
                for row in range(2 * heads):
                    line_ref[number * size + first + offset, row] = made[row]
            return top

        top = lax.fori_loop(0, size // SCORE_UNROLL, score_step, top)
    top_ref[...] = top

    def tile_sum(place):
        entry = list_ref[part, jnp.minimum(place, list_ref.shape[1] - 1)]
        block = (entry >> 8) & (BLOCKS - 1)
        spot = entry >> 11
        keep = masks_ref[jnp.where(place < live, entry & 255, masks_ref.shape[0] - 1)]
        left = []
        for head in range(heads):
            up = wide_row(line_ref[spot, head], rows)
            down = wide_row(line_ref[spot, heads + head], rows)
            left.append(jnp.maximum(up, ratio_ref[block, head].astype(jnp.bfloat16) * down) * keep)
        return block, tile_product(left, values_ref[spot].astype(jnp.bfloat16), heads_ref)

    def tile_round(index, carry):
        first = index * TILE_UNROLL
        sums = [tile_sum(first + offset) for offset in range(TILE_UNROLL)]
        for block, total in sums:
            acc_ref[block] += total
        return carry

    lax.fori_loop(0, rounds, tile_round, 0)


def step_kernel(part, list_ref, masks_ref, ratio_ref, init_ref, peak_ref, att_ref, heads_ref, *refs):
    pieces, (acc_ref, top_ref), scratch = refs[:-4], refs[-4:-2], refs[-2:]
    half_pass(part, list_ref, masks_ref, pieces, ratio_ref, att_ref, heads_ref, acc_ref, top_ref, *scratch)


def half_scratch(rows, feats, heads, pieces):
    slots = len(pieces) * pieces[0].shape[0]
    return [
        pltpu.VMEM((slots, 2 * heads, 8, feats), jnp.float32),
        pltpu.VMEM((slots, rows, feats), jnp.float32),
    ]


def attend_step(part, tile_rows, masks, ratio, acc, top, att3, head_rows, pieces):
    num_blocks, heads, rows, _ = ratio.shape
    feats = att3.shape[1]
    return pl.pallas_call(
        functools.partial(step_kernel, part),
        in_specs=[pl.BlockSpec(memory_space=pltpu.SMEM)]
        + [pl.BlockSpec(memory_space=pltpu.VMEM)] * (6 + len(pieces)),
        out_specs=[pl.BlockSpec(memory_space=pltpu.VMEM)] * 2,
        out_shape=[
            jax.ShapeDtypeStruct((num_blocks, rows, 2 * feats), jnp.float32),
            jax.ShapeDtypeStruct((8, feats), jnp.float32),
        ],
        scratch_shapes=half_scratch(rows, feats, heads, pieces),
        compiler_params=pltpu.CompilerParams(vmem_limit_bytes=10 * 1024 * 1024),
        cost_estimate=pl.CostEstimate(flops=6 * 10**9, bytes_accessed=8 * 10**6, transcendentals=10**6),
        input_output_aliases={3: 0, 4: 1},
        name="attend_step",
    )(tile_rows, masks, ratio, acc, top, att3, head_rows, *pieces)


def last_kernel(
    part,
    list_ref,
    masks_ref,
    ratio_ref,
    init_ref,
    peak_ref,
    att_ref,
    heads_ref,
    bias_ref,
    dst_ref,
    spot_ref,
    count_ref,
    att_src_ref,
    att_dst_ref,
    own_hbm,
    *refs,
):
    early, pieces, out_ref = refs[:-12], refs[-12:-10], refs[-10]
    acc_ref, top_ref, line_ref, values_ref, own_ref, far_ref, slow_dst, slow_peak, slow_sem = refs[-9:]
    acc_ref[...] = init_ref[...]
    top_ref[...] = peak_ref[...]
    half_pass(part, list_ref, masks_ref, pieces, ratio_ref, att_ref, heads_ref, acc_ref, top_ref, line_ref, values_ref)
    num_blocks, rows, feats = out_ref.shape
    heads = heads_ref.shape[0]
    in_range = jnp.max(top_ref[...]) <= LIMIT

    def finish(block, sums):
        mixed = sums[:, :feats] / sums[:, feats:] + bias_ref[...]
        out_ref[block] = elu(mixed).astype(out_ref.dtype)

    for block in range(num_blocks):
        finish(block, acc_ref[block])

    @pl.when(jnp.logical_not(in_range))
    def _():
        live = count_ref[0]

        def load(source, target):
            copy = pltpu.make_async_copy(source, target, slow_sem)
            copy.start()
            copy.wait()

        load(own_hbm.at[pl.ds(0, num_blocks)], own_ref)
        src_table = head_table(att_src_ref[...])
        dst_table = head_table(att_dst_ref[...])
        width = att_src_ref.shape[1]
        size = SIDE * SIDE
        for index, piece in enumerate(early + pieces):
            load(piece, far_ref.at[pl.ds(index * size, size)])

        def set_block(block, carry):
            own = own_ref[block]
            wide = wide_scores(own, dst_table, rows)
            src_own = wide_scores(own, src_table, width)
            for head in range(heads):
                slow_dst[block, head] = wide[:, head * rows : (head + 1) * rows]
                first = head * (feats // heads)
                slow_peak[block, head] = jnp.broadcast_to(src_own[:, first : first + 1], (rows, rows))
            return carry

        lax.fori_loop(0, num_blocks, set_block, 0)

        def peak_tile(tile, carry):
            block = dst_ref[0, tile]
            scores = source_scores(att_ref, far_ref[spot_ref[0, tile]], heads)
            keep = masks_ref[tile].astype(jnp.float32) > 0
            for head in range(heads):
                kept = jnp.where(keep, jnp.broadcast_to(scores[head : head + 1, :], (rows, rows)), -jnp.inf)
                tile_top = jnp.max(kept, axis=1, keepdims=True)
                slow_peak[block, head] = jnp.maximum(slow_peak[block, head], tile_top)
            return carry

        lax.fori_loop(0, live, peak_tile, 0)

        def self_block(block, carry):
            own = own_ref[block]
            src_own = wide_scores(own, src_table, width)
            dst_own = wide_scores(own, dst_table, width)
            lane_head = lax.broadcasted_iota(jnp.int32, (rows, feats), 1) // (feats // heads)
            top = jnp.zeros((rows, feats), jnp.float32)
            for head in range(heads):
                peak = leaky_relu(slow_dst[block, head] + slow_peak[block, head])
                slow_peak[block, head] = peak
                top = jnp.where(lane_head == head, peak, top)
            self_weight = jnp.exp(leaky_relu(dst_own + src_own) - top)
            rounded = self_weight.astype(jnp.bfloat16).astype(jnp.float32)
            acc_ref[block, :, :feats] = rounded * own.astype(jnp.float32)
            acc_ref[block, :, feats:] = self_weight
            return carry

        lax.fori_loop(0, num_blocks, self_block, 0)

        def slow_tile(tile, carry):
            block = dst_ref[0, tile]
            values = far_ref[spot_ref[0, tile]]
            scores = source_scores(att_ref, values, heads)
            keep = masks_ref[tile].astype(jnp.float32) > 0
            left = []
            for head in range(heads):
                logit = leaky_relu(slow_dst[block, head] + scores[head : head + 1, :])
                shifted = jnp.where(keep, logit - slow_peak[block, head], -jnp.inf)
                left.append(jnp.exp(shifted).astype(jnp.bfloat16))
            acc_ref[block] += tile_product(left, values, heads_ref)
            return carry

        lax.fori_loop(0, live, slow_tile, 0)
        for block in range(num_blocks):
            finish(block, acc_ref[block])


def attend_last(lists, masks, ratio, acc, top, att3, head_rows, bias, scalars, atts, own_proj, early, pieces):
    num_blocks, heads, rows, _ = ratio.shape
    feats = att3.shape[1]
    vmem = pl.BlockSpec(memory_space=pltpu.VMEM)
    smem = pl.BlockSpec(memory_space=pltpu.SMEM)
    return pl.pallas_call(
        functools.partial(last_kernel, len(GROUPS) - 1),
        in_specs=[smem]
        + [vmem] * 7
        + [smem] * 3
        + [vmem] * 2
        + [pl.BlockSpec(memory_space=pl.ANY)] * (1 + len(early))
        + [vmem] * len(pieces),
        out_specs=vmem,
        out_shape=jax.ShapeDtypeStruct((num_blocks, rows, feats), jnp.bfloat16),
        scratch_shapes=[pltpu.VMEM(acc.shape, acc.dtype), pltpu.VMEM(top.shape, top.dtype)]
        + half_scratch(rows, feats, heads, pieces)
        + [
            pltpu.VMEM((num_blocks, rows, feats), jnp.bfloat16),
            pltpu.VMEM((2 * SIDE**3, rows, feats), jnp.bfloat16),
            pltpu.VMEM((num_blocks, heads, rows, rows), jnp.float32),
            pltpu.VMEM((num_blocks, heads, rows, rows), jnp.float32),
            pltpu.SemaphoreType.DMA,
        ],
        compiler_params=pltpu.CompilerParams(vmem_limit_bytes=20 * 1024 * 1024),
        cost_estimate=pl.CostEstimate(flops=7 * 10**9, bytes_accessed=8 * 10**6, transcendentals=10**6),
        name="attend_last",
    )(lists, masks, ratio, acc, top, att3, head_rows, bias, *scalars, *atts, own_proj, *early, *pieces)


def local(
    node_feats,
    weight,
    att_src,
    att_dst,
    out_bias,
    requests,
    tile_dst,
    tile_src,
    tile_masks,
    tile_count,
):
    feats = att_src.size
    rows = tile_masks.shape[2]
    num_blocks = node_feats.shape[0] // rows
    device = lax.axis_index("node").astype(jnp.int32).reshape(1)

    pair = pair_rows(requests, shift_along(requests, 0, 0, 1))
    lines = spread(pair, 2)
    own, staged = project_own(node_feats, weight)
    low, high = project(own, spread(node_feats, 0)[1:], staged, lines[1:])
    left_low = shift_along(low, 1, 1)
    right_high = shift_along(high, 1, 3)
    left_high = shift_along(high, 1, 1)
    right_low = shift_along(low, 1, 3)
    far_low = shift_along(left_low, 1, 1)
    far_high = shift_along(right_high, 1, 3)
    planes = [low, high, left_low, left_high, far_low, far_high, right_low, right_high]
    own_blocks = own.reshape(num_blocks, rows, feats)

    masks = stage_masks(tile_count, tile_masks)
    lists, spots = ready(device, tile_dst, tile_src, tile_count)
    ratio, init, peak, att3, picks = prep(own_blocks, att_src, att_dst)

    held = lax.optimization_barrier((planes, lines, ratio, init, peak, att3, picks, lists, spots, masks))
    planes, lines, ratio, init, peak, att3, picks, lists, spots, masks = held
    picked = pick_blocks(device, lines, planes)
    arrived = {(hop, half): picked[2 * hop + half] for hop in range(SIDE) for half in range(2)}
    arrived[0, 1] = shift_along(arrived[0, 1], 2, 0, 1)
    for hop, half in ((2, 0), (2, 1), (1, 0), (3, 0), (1, 1), (3, 1)):
        arrived[hop, half] = shift_along(arrived[hop, half], 2, hop, half)
    landed = [[arrived[key] for key in keys] for keys in GROUPS]

    acc, top = init, peak
    for part in range(len(GROUPS) - 1):
        acc, top = attend_step(part, lists, masks, ratio, acc, top, att3, picks, landed[part])
    out = attend_last(
        lists,
        masks,
        ratio,
        acc,
        top,
        att3,
        picks,
        out_bias.reshape(1, feats),
        (tile_dst, spots, tile_count),
        (att_src, att_dst),
        own_blocks,
        sum(landed[:-1], []),
        landed[-1],
    )
    return out.reshape(num_blocks * rows, feats)


def solution(mesh):
    placed = (
        P("node", None),
        P(),
        P(),
        P(),
        P(),
        P("node", None),
        P("node", None),
        P("node", None),
        P("node", None, None, None),
        P("node"),
    )
    return jax.shard_map(
        local, mesh=mesh, in_specs=placed, out_specs=P("node", None), check_vma=False
    )
```

```python
import functools

import jax
import jax.numpy as jnp
from jax import lax
from jax.experimental import pallas as pl
from jax.experimental.pallas import tpu as pltpu
from jax.sharding import PartitionSpec as P

LIMIT = 40.0
PACK = 16
STAGE = 8
SCORE_UNROLL = 16
TILE_UNROLL = 8
REST_UNROLL = 4
SIDE = 4
BLOCKS = 8
STRIDE = (32, 8, 2)
SHIFT = (5, 3, 1)
ROTATION = ((2, 0, 1), (0, 1, 2))
GROUPS = (((0, 0), (0, 1)), ((2, 0), (2, 1)), ((1, 0), (3, 0)), ((1, 1), (3, 1)))


def split3(table):
    high = table.astype(jnp.bfloat16)
    rest = table - high.astype(jnp.float32)
    mid = rest.astype(jnp.bfloat16)
    low = (rest - mid.astype(jnp.float32)).astype(jnp.bfloat16)
    return high, mid, low


def head_table(att):
    heads, width = att.shape
    tiled = jnp.concatenate([att] * heads, axis=1)
    lane_head = lax.broadcasted_iota(jnp.int32, tiled.shape, 1) // width
    return jnp.where(lane_head == lax.broadcasted_iota(jnp.int32, tiled.shape, 0), tiled, 0.0)


def wide_scores(values, table, repeat):
    heads, feats = table.shape
    spread_rows = jnp.concatenate(
        [jnp.broadcast_to(table[head : head + 1], (repeat, feats)) for head in range(heads)], axis=0
    )
    high, mid, low = split3(spread_rows)
    return dot_nt(values, high) + dot_nt(values, mid) + dot_nt(values, low)


def leaky_relu(in_value):
    return jnp.where(in_value > 0, in_value, 0.2 * in_value)


def elu(in_value):
    return jnp.where(in_value > 0, in_value, jnp.exp(jnp.minimum(in_value, 0.0)) - 1.0)


def dot_f32(left, right):
    return jnp.dot(left, right, preferred_element_type=jnp.float32)


def dot_nt(left, right):
    return lax.dot_general(left, right, (((1,), (1,)), ((), ())), preferred_element_type=jnp.float32)


def stage_kernel(feats_ref, weight_ref, own_ref, weight_copy):
    own_ref[...] = dot_f32(feats_ref[...], weight_ref[...]).astype(own_ref.dtype)
    weight_copy[...] = weight_ref[...]


def project_own(node_feats, weight):
    return pl.pallas_call(
        stage_kernel,
        out_shape=[
            jax.ShapeDtypeStruct((node_feats.shape[0], weight.shape[1]), jnp.bfloat16),
            jax.ShapeDtypeStruct(weight.shape, weight.dtype),
        ],
        compiler_params=pltpu.CompilerParams(vmem_limit_bytes=8 * 1024 * 1024),
        cost_estimate=pl.CostEstimate(flops=10**9, bytes_accessed=10**6, transcendentals=0),
        name="project_own",
    )(node_feats, weight)


def pair_kernel(own_ref, partner_ref, out_ref):
    out_ref[0:1] = own_ref[...]
    out_ref[1:2] = partner_ref[...]


def pair_rows(own, partner):
    return pl.pallas_call(
        pair_kernel,
        out_shape=jax.ShapeDtypeStruct((2, own.shape[1]), own.dtype),
        compiler_params=pltpu.CompilerParams(vmem_limit_bytes=1024 * 1024),
        name="pair_rows",
    )(own, partner)


def project_kernel(weight_ref, own_ref, piece1, piece2, piece3, *refs):
    low_ref, high_ref = refs[-2:]
    _, rows, feats = low_ref.shape
    project_one = lambda piece: dot_f32(piece[...], weight_ref[...]).astype(low_ref.dtype)
    low_ref[:BLOCKS] = own_ref[...].reshape(BLOCKS, rows, feats)
    low_ref[BLOCKS:] = project_one(piece1).reshape(BLOCKS, rows, feats)
    high_ref[:BLOCKS] = project_one(piece2).reshape(BLOCKS, rows, feats)
    high_ref[BLOCKS:] = project_one(piece3).reshape(BLOCKS, rows, feats)


def project(own, pieces, weight, after):
    rows = own.shape[0] // BLOCKS
    feats = weight.shape[1]
    return pl.pallas_call(
        project_kernel,
        in_specs=[pl.BlockSpec(memory_space=pltpu.VMEM)] * 5 + [pl.BlockSpec(memory_space=pl.ANY)] * len(after),
        out_shape=[jax.ShapeDtypeStruct((SIDE * BLOCKS // 2, rows, feats), jnp.bfloat16)] * 2,
        compiler_params=pltpu.CompilerParams(vmem_limit_bytes=8 * 1024 * 1024),
        cost_estimate=pl.CostEstimate(flops=2 * 10**9, bytes_accessed=2 * 10**6, transcendentals=0),
        name="project",
    )(weight, own, *pieces, *after)


def by_core(core, pair):
    return jnp.where(core == 0, pair[0], pair[1])


def place_of(device):
    core = device & 1
    place = [(device >> shift) & (SIDE - 1) for shift in SHIFT]
    here = [by_core(core, [place[ROTATION[owner][phase]] for owner in range(2)]) for phase in range(3)]
    step = [by_core(core, [STRIDE[ROTATION[owner][phase]] for owner in range(2)]) for phase in range(3)]
    return core, place, here, step


def pick_kernel(device_ref, *refs):
    lines, pieces, outs = refs[:SIDE], refs[SIDE : 3 * SIDE], refs[3 * SIDE :]
    core, _, here, step = place_of(device_ref[0])
    for second in range(SIDE):
        for first in range(SIDE):
            peer = (
                ((here[0] - first) & (SIDE - 1)) * step[0]
                + ((here[1] - second) & (SIDE - 1)) * step[1]
                + here[2] * step[2]
                + core
            )
            piece = pieces[second * 2 + first // 2]
            for hop in range(SIDE):
                for half in range(2):
                    chosen = lines[(SIDE - hop) % SIDE][half, peer]
                    outs[hop * 2 + half][second * SIDE + first] = piece[first % 2 * BLOCKS + chosen]


def pick_blocks(device, lines, pieces):
    rows, feats = pieces[0].shape[1:]
    return pl.pallas_call(
        pick_kernel,
        in_specs=[pl.BlockSpec(memory_space=pltpu.SMEM)] * (1 + SIDE)
        + [pl.BlockSpec(memory_space=pltpu.VMEM)] * (2 * SIDE),
        out_specs=[pl.BlockSpec(memory_space=pltpu.VMEM)] * (2 * SIDE),
        out_shape=[jax.ShapeDtypeStruct((SIDE * SIDE, rows, feats), jnp.bfloat16)] * (2 * SIDE),
        compiler_params=pltpu.CompilerParams(vmem_limit_bytes=12 * 1024 * 1024),
        cost_estimate=pl.CostEstimate(flops=2 * 10**8, bytes_accessed=4 * 10**6, transcendentals=0),
        name="pick_blocks",
    )(device, *lines, *pieces)


def route(axes, shift, swap=0):
    pairs = []
    for device in range(2 * SIDE**3):
        stride = STRIDE[axes[device % 2]]
        place = device // stride % SIDE
        target = device + ((place + shift) % SIDE - place) * stride
        pairs.append((device, target ^ swap))
    return pairs


def shift_along(value, phase, shift, swap=0):
    axes = tuple(ROTATION[core][phase] for core in range(2))
    return lax.ppermute(value, "node", route(axes, shift, swap))


def spread(value, phase):
    moved = {hop: shift_along(value, phase, hop) for hop in (2, 1, 3)}
    return [value] + [moved[hop] for hop in range(1, SIDE)]


def ready_kernel(device_ref, count_ref, dst_ref, src_ref, list_ref, spot_ref):
    tiles = src_ref.shape[1]
    core, place, _, _ = place_of(device_ref[0])
    peer = src_ref[...]
    away = [(place[axis] - (peer >> SHIFT[axis])) & (SIDE - 1) for axis in range(3)]
    owner = peer & 1
    first, second, third = [
        jnp.where(owner == 0, away[ROTATION[0][phase]], away[ROTATION[1][phase]]) for phase in range(3)
    ]
    half = owner ^ core
    even = (third & 1) == 0
    group = jnp.where(even, third >> 1, 2 + half)
    local_spot = (jnp.where(even, half, third >> 1) * SIDE + second) * SIDE + first
    spot_ref[...] = group * 2 * SIDE * SIDE + local_spot
    tile = lax.broadcasted_iota(jnp.int32, (1, tiles), 1)
    group = jnp.where(tile < count_ref[0], group, 8)
    one = lambda hit: jnp.where(hit, 1.0, 0.0)
    member = one(lax.broadcasted_iota(jnp.int32, (8, tiles), 0) == group)
    up = lax.broadcasted_iota(jnp.int32, (tiles, tiles), 0)
    across = lax.broadcasted_iota(jnp.int32, (tiles, tiles), 1)
    before = dot_f32(member.astype(jnp.bfloat16), one(up < across).astype(jnp.bfloat16))
    rank = jnp.sum(member * before, axis=0, keepdims=True).astype(jnp.int32)
    row = lax.broadcasted_iota(jnp.int32, (8, tiles), 0)
    facts = jnp.where(row == 0, tile, jnp.where(row == 1, dst_ref[...] + 8 * local_spot, 0))
    facts = facts.astype(jnp.float32).astype(jnp.bfloat16)
    for part in range(len(GROUPS)):
        hit = (rank == up) & (group == part)
        found = dot_nt(facts, one(hit).astype(jnp.bfloat16))
        list_ref[part : part + 1] = (found[0:1] + 256.0 * found[1:2]).astype(jnp.int32)
    total = jnp.sum(member, axis=1, keepdims=True).astype(jnp.int32)
    list_ref[8:16] = jnp.broadcast_to(total, (8, tiles))


def ready(device, tile_dst, tile_src, tile_count):
    tiles = tile_src.shape[1]
    smem = pl.BlockSpec(memory_space=pltpu.SMEM)
    vmem = pl.BlockSpec(memory_space=pltpu.VMEM)
    return pl.pallas_call(
        ready_kernel,
        in_specs=[smem, smem, vmem, vmem],
        out_specs=[vmem, vmem],
        out_shape=[
            jax.ShapeDtypeStruct((16, tiles), jnp.int32),
            jax.ShapeDtypeStruct((1, tiles), jnp.int32),
        ],
        compiler_params=pltpu.CompilerParams(vmem_limit_bytes=4 * 1024 * 1024),
        cost_estimate=pl.CostEstimate(flops=10**9, bytes_accessed=10**5, transcendentals=0),
        name="ready",
    )(device, tile_count, tile_dst, tile_src)


def masks_kernel(count_ref, mask_hbm, out_ref, stage_ref, sems):
    tiles = mask_hbm.shape[1]
    rounds = (count_ref[0] + STAGE - 1) // STAGE

    def stage_copy(index):
        source = mask_hbm.at[0, pl.ds(index * STAGE, STAGE)]
        return pltpu.make_async_copy(source, stage_ref.at[index & 3], sems.at[index & 3])

    for index in range(3):

        @pl.when(index < rounds)
        def _():
            stage_copy(index).start()

    out_ref[tiles] = jnp.zeros(out_ref.shape[1:], out_ref.dtype)

    def stage_round(index, carry):
        @pl.when(index + 3 < rounds)
        def _():
            stage_copy(index + 3).start()

        stage_copy(index).wait()
        for offset in range(STAGE):
            out_ref[index * STAGE + offset] = stage_ref[index & 3, offset].astype(jnp.float32).astype(out_ref.dtype)
        return carry

    lax.fori_loop(0, rounds, stage_round, 0)


def stage_masks(tile_count, masks):
    _, tiles, rows, _ = masks.shape
    return pl.pallas_call(
        masks_kernel,
        in_specs=[pl.BlockSpec(memory_space=pltpu.SMEM), pl.BlockSpec(memory_space=pl.ANY)],
        out_specs=pl.BlockSpec(memory_space=pltpu.VMEM),
        out_shape=jax.ShapeDtypeStruct((tiles + 1, rows, rows), jnp.bfloat16),
        scratch_shapes=[pltpu.VMEM((4, STAGE, rows, rows), jnp.int32), pltpu.SemaphoreType.DMA((4,))],
        compiler_params=pltpu.CompilerParams(vmem_limit_bytes=48 * 1024 * 1024),
        cost_estimate=pl.CostEstimate(flops=3 * 10**9, bytes_accessed=12 * 10**6, transcendentals=0),
        name="stage_masks",
    )(tile_count, masks)


def prep_kernel(own_ref, att_src_ref, att_dst_ref, ratio_ref, acc_ref, peak_ref, att_ref, heads_ref):
    own = own_ref[0]
    heads = ratio_ref.shape[1]
    rows = own.shape[0]
    src_table = head_table(att_src_ref[...])
    dst_table = head_table(att_dst_ref[...])
    att_ref[...] = jnp.concatenate([part.astype(jnp.float32) for part in split3(src_table)], axis=0)
    lane_head = lax.broadcasted_iota(jnp.int32, (8, own.shape[1]), 1) // att_src_ref.shape[1]
    for head in range(heads):
        heads_ref[head] = jnp.where(lane_head == head, 1.0, 0.0)
    ratio = jnp.exp(-0.8 * wide_scores(own, dst_table, rows))
    for head in range(heads):
        ratio_ref[0, head] = ratio[:, head * rows : (head + 1) * rows]
    src_own = wide_scores(own, src_table, att_src_ref.shape[1])
    dst_own = wide_scores(own, dst_table, att_src_ref.shape[1])
    self_weight = jnp.maximum(jnp.exp(src_own), jnp.exp(0.2 * src_own - 0.8 * dst_own))
    rounded = self_weight.astype(jnp.bfloat16).astype(jnp.float32)
    feats = own.shape[1]
    acc_ref[0, :, :feats] = rounded * own.astype(jnp.float32)
    acc_ref[0, :, feats:] = self_weight
    size = jnp.maximum(jnp.abs(src_own), jnp.abs(dst_own)).reshape(rows // 8, 8, feats)

    @pl.when(pl.program_id(0) == 0)
    def _():
        peak_ref[...] = jnp.zeros_like(peak_ref)

    peak_ref[...] = jnp.maximum(peak_ref[...], jnp.max(size, axis=0))


def prep(own_proj, att_src, att_dst):
    _, rows, feats = own_proj.shape
    heads = att_src.shape[0]
    whole = lambda b: (0, 0)
    return pl.pallas_call(
        prep_kernel,
        grid=(BLOCKS,),
        in_specs=[
            pl.BlockSpec((1, rows, feats), lambda b: (b, 0, 0)),
            pl.BlockSpec(att_src.shape, whole),
            pl.BlockSpec(att_dst.shape, whole),
        ],
        out_specs=[
            pl.BlockSpec((1, heads, rows, rows), lambda b: (b, 0, 0, 0)),
            pl.BlockSpec((1, rows, 2 * feats), lambda b: (b, 0, 0)),
            pl.BlockSpec((8, feats), whole),
            pl.BlockSpec((3 * heads, feats), whole),
            pl.BlockSpec((heads, 8, feats), lambda b: (0, 0, 0)),
        ],
        out_shape=[
            jax.ShapeDtypeStruct((BLOCKS, heads, rows, rows), jnp.float32),
            jax.ShapeDtypeStruct((BLOCKS, rows, 2 * feats), jnp.float32),
            jax.ShapeDtypeStruct((8, feats), jnp.float32),
            jax.ShapeDtypeStruct((3 * heads, feats), jnp.float32),
            jax.ShapeDtypeStruct((heads, 8, feats), jnp.float32),
        ],
        compiler_params=pltpu.CompilerParams(vmem_limit_bytes=16 * 1024 * 1024),
        cost_estimate=pl.CostEstimate(flops=3 * 10**9, bytes_accessed=4 * 10**6, transcendentals=10**6),
        name="prep",
    )(own_proj, att_src, att_dst)


def source_scores(att_ref, values, heads):
    parts = dot_nt(att_ref[...].astype(jnp.bfloat16), values)
    return parts[0:heads] + parts[heads : 2 * heads] + parts[2 * heads : 3 * heads]


def wide_row(row, rows):
    pair = jnp.concatenate([row] * (PACK // row.shape[0]), axis=0).astype(jnp.bfloat16)
    return jnp.concatenate([pair] * (rows // PACK), axis=0)


def tile_product(left, values, heads_ref):
    rows = values.shape[0]
    right = []
    for head in range(len(left)):
        pick = wide_row(heads_ref[head], rows)
        right.append(jnp.concatenate([values * pick, pick], axis=1))
    return dot_f32(jnp.concatenate(left, axis=1), jnp.concatenate(right, axis=0))


def half_pass(part, list_ref, masks_ref, pieces, ratio_ref, att_ref, heads_ref, acc_ref, top_ref, line_ref, values_ref):
    _, heads, rows, _ = ratio_ref.shape
    feats = values_ref.shape[2]
    size = SIDE * SIDE
    live = list_ref[8 + part, 0]
    full = live // TILE_UNROLL
    rest = (live - full * TILE_UNROLL + REST_UNROLL - 1) // REST_UNROLL

    def weight_rows(piece, slot, from_slot):
        block_values = piece[from_slot]
        values_ref[slot] = block_values.astype(jnp.float32)
        scores = source_scores(att_ref, block_values, heads)
        made = []
        for values in (jnp.exp(scores), jnp.exp(0.2 * scores)):
            for head in range(heads):
                made.append(jnp.broadcast_to(values[head : head + 1, :], (8, feats)))
        return jnp.abs(scores), made

    top = top_ref[...]
    for number, piece in enumerate(pieces):

        def score_step(index, top):
            first = index * SCORE_UNROLL
            all_made = [
                weight_rows(piece, number * size + first + offset, first + offset) for offset in range(SCORE_UNROLL)
            ]
            for offset, (extent, made) in enumerate(all_made):
                top = jnp.maximum(top, extent)
                for row in range(2 * heads):
                    line_ref[number * size + first + offset, row] = made[row]
            return top

        top = lax.fori_loop(0, size // SCORE_UNROLL, score_step, top)
    top_ref[...] = top

    def tile_sum(place):
        entry = list_ref[part, jnp.minimum(place, list_ref.shape[1] - 1)]
        block = (entry >> 8) & (BLOCKS - 1)
        spot = entry >> 11
        keep = masks_ref[jnp.where(place < live, entry & 255, masks_ref.shape[0] - 1)]
        left = []
        for head in range(heads):
            up = wide_row(line_ref[spot, head], rows)
            down = wide_row(line_ref[spot, heads + head], rows)
            left.append(jnp.maximum(up, ratio_ref[block, head].astype(jnp.bfloat16) * down) * keep)
        return block, tile_product(left, values_ref[spot].astype(jnp.bfloat16), heads_ref)

    def add_tiles(first, count):
        sums = [tile_sum(first + offset) for offset in range(count)]
        for block, total in sums:
            acc_ref[block] += total

    def full_round(index, carry):
        add_tiles(index * TILE_UNROLL, TILE_UNROLL)
        return carry

    def rest_round(index, carry):
        add_tiles(full * TILE_UNROLL + index * REST_UNROLL, REST_UNROLL)
        return carry

    lax.fori_loop(0, full, full_round, 0)
    lax.fori_loop(0, rest, rest_round, 0)


def step_kernel(part, list_ref, masks_ref, ratio_ref, init_ref, peak_ref, att_ref, heads_ref, *refs):
    pieces, (acc_ref, top_ref), scratch = refs[:-4], refs[-4:-2], refs[-2:]
    half_pass(part, list_ref, masks_ref, pieces, ratio_ref, att_ref, heads_ref, acc_ref, top_ref, *scratch)


def half_scratch(rows, feats, heads, pieces):
    slots = len(pieces) * pieces[0].shape[0]
    return [
        pltpu.VMEM((slots, 2 * heads, 8, feats), jnp.float32),
        pltpu.VMEM((slots, rows, feats), jnp.float32),
    ]


def attend_step(part, tile_rows, masks, ratio, acc, top, att3, head_rows, pieces):
    num_blocks, heads, rows, _ = ratio.shape
    feats = att3.shape[1]
    return pl.pallas_call(
        functools.partial(step_kernel, part),
        in_specs=[pl.BlockSpec(memory_space=pltpu.SMEM)]
        + [pl.BlockSpec(memory_space=pltpu.VMEM)] * (6 + len(pieces)),
        out_specs=[pl.BlockSpec(memory_space=pltpu.VMEM)] * 2,
        out_shape=[
            jax.ShapeDtypeStruct((num_blocks, rows, 2 * feats), jnp.float32),
            jax.ShapeDtypeStruct((8, feats), jnp.float32),
        ],
        scratch_shapes=half_scratch(rows, feats, heads, pieces),
        compiler_params=pltpu.CompilerParams(vmem_limit_bytes=10 * 1024 * 1024),
        cost_estimate=pl.CostEstimate(flops=6 * 10**9, bytes_accessed=8 * 10**6, transcendentals=10**6),
        input_output_aliases={3: 0, 4: 1},
        name="attend_step",
    )(tile_rows, masks, ratio, acc, top, att3, head_rows, *pieces)


def last_kernel(
    part,
    list_ref,
    masks_ref,
    ratio_ref,
    init_ref,
    peak_ref,
    att_ref,
    heads_ref,
    bias_ref,
    dst_ref,
    spot_ref,
    count_ref,
    att_src_ref,
    att_dst_ref,
    own_hbm,
    *refs,
):
    early, pieces, out_ref = refs[:-12], refs[-12:-10], refs[-10]
    acc_ref, top_ref, line_ref, values_ref, own_ref, far_ref, slow_dst, slow_peak, slow_sem = refs[-9:]
    acc_ref[...] = init_ref[...]
    top_ref[...] = peak_ref[...]
    half_pass(part, list_ref, masks_ref, pieces, ratio_ref, att_ref, heads_ref, acc_ref, top_ref, line_ref, values_ref)
    num_blocks, rows, feats = out_ref.shape
    heads = heads_ref.shape[0]
    in_range = jnp.max(top_ref[...]) <= LIMIT

    def finish(block, sums):
        mixed = sums[:, :feats] / sums[:, feats:] + bias_ref[...]
        out_ref[block] = elu(mixed).astype(out_ref.dtype)

    for block in range(num_blocks):
        finish(block, acc_ref[block])

    @pl.when(jnp.logical_not(in_range))
    def _():
        live = count_ref[0]

        def load(source, target):
            copy = pltpu.make_async_copy(source, target, slow_sem)
            copy.start()
            copy.wait()

        load(own_hbm.at[pl.ds(0, num_blocks)], own_ref)
        src_table = head_table(att_src_ref[...])
        dst_table = head_table(att_dst_ref[...])
        width = att_src_ref.shape[1]
        size = SIDE * SIDE
        for index, piece in enumerate(early + pieces):
            load(piece, far_ref.at[pl.ds(index * size, size)])

        def set_block(block, carry):
            own = own_ref[block]
            wide = wide_scores(own, dst_table, rows)
            src_own = wide_scores(own, src_table, width)
            for head in range(heads):
                slow_dst[block, head] = wide[:, head * rows : (head + 1) * rows]
                first = head * (feats // heads)
                slow_peak[block, head] = jnp.broadcast_to(src_own[:, first : first + 1], (rows, rows))
            return carry

        lax.fori_loop(0, num_blocks, set_block, 0)

        def peak_tile(tile, carry):
            block = dst_ref[0, tile]
            scores = source_scores(att_ref, far_ref[spot_ref[0, tile]], heads)
            keep = masks_ref[tile].astype(jnp.float32) > 0
            for head in range(heads):
                kept = jnp.where(keep, jnp.broadcast_to(scores[head : head + 1, :], (rows, rows)), -jnp.inf)
                tile_top = jnp.max(kept, axis=1, keepdims=True)
                slow_peak[block, head] = jnp.maximum(slow_peak[block, head], tile_top)
            return carry

        lax.fori_loop(0, live, peak_tile, 0)

        def self_block(block, carry):
            own = own_ref[block]
            src_own = wide_scores(own, src_table, width)
            dst_own = wide_scores(own, dst_table, width)
            lane_head = lax.broadcasted_iota(jnp.int32, (rows, feats), 1) // (feats // heads)
            top = jnp.zeros((rows, feats), jnp.float32)
            for head in range(heads):
                peak = leaky_relu(slow_dst[block, head] + slow_peak[block, head])
                slow_peak[block, head] = peak
                top = jnp.where(lane_head == head, peak, top)
            self_weight = jnp.exp(leaky_relu(dst_own + src_own) - top)
            rounded = self_weight.astype(jnp.bfloat16).astype(jnp.float32)
            acc_ref[block, :, :feats] = rounded * own.astype(jnp.float32)
            acc_ref[block, :, feats:] = self_weight
            return carry

        lax.fori_loop(0, num_blocks, self_block, 0)

        def slow_tile(tile, carry):
            block = dst_ref[0, tile]
            values = far_ref[spot_ref[0, tile]]
            scores = source_scores(att_ref, values, heads)
            keep = masks_ref[tile].astype(jnp.float32) > 0
            left = []
            for head in range(heads):
                logit = leaky_relu(slow_dst[block, head] + scores[head : head + 1, :])
                shifted = jnp.where(keep, logit - slow_peak[block, head], -jnp.inf)
                left.append(jnp.exp(shifted).astype(jnp.bfloat16))
            acc_ref[block] += tile_product(left, values, heads_ref)
            return carry

        lax.fori_loop(0, live, slow_tile, 0)
        for block in range(num_blocks):
            finish(block, acc_ref[block])


def attend_last(lists, masks, ratio, acc, top, att3, head_rows, bias, scalars, atts, own_proj, early, pieces):
    num_blocks, heads, rows, _ = ratio.shape
    feats = att3.shape[1]
    vmem = pl.BlockSpec(memory_space=pltpu.VMEM)
    smem = pl.BlockSpec(memory_space=pltpu.SMEM)
    return pl.pallas_call(
        functools.partial(last_kernel, len(GROUPS) - 1),
        in_specs=[smem]
        + [vmem] * 7
        + [smem] * 3
        + [vmem] * 2
        + [pl.BlockSpec(memory_space=pl.ANY)] * (1 + len(early))
        + [vmem] * len(pieces),
        out_specs=vmem,
        out_shape=jax.ShapeDtypeStruct((num_blocks, rows, feats), jnp.bfloat16),
        scratch_shapes=[pltpu.VMEM(acc.shape, acc.dtype), pltpu.VMEM(top.shape, top.dtype)]
        + half_scratch(rows, feats, heads, pieces)
        + [
            pltpu.VMEM((num_blocks, rows, feats), jnp.bfloat16),
            pltpu.VMEM((2 * SIDE**3, rows, feats), jnp.bfloat16),
            pltpu.VMEM((num_blocks, heads, rows, rows), jnp.float32),
            pltpu.VMEM((num_blocks, heads, rows, rows), jnp.float32),
            pltpu.SemaphoreType.DMA,
        ],
        compiler_params=pltpu.CompilerParams(vmem_limit_bytes=20 * 1024 * 1024),
        cost_estimate=pl.CostEstimate(flops=7 * 10**9, bytes_accessed=8 * 10**6, transcendentals=10**6),
        name="attend_last",
    )(lists, masks, ratio, acc, top, att3, head_rows, bias, *scalars, *atts, own_proj, *early, *pieces)


def local(
    node_feats,
    weight,
    att_src,
    att_dst,
    out_bias,
    requests,
    tile_dst,
    tile_src,
    tile_masks,
    tile_count,
):
    feats = att_src.size
    rows = tile_masks.shape[2]
    num_blocks = node_feats.shape[0] // rows
    device = lax.axis_index("node").astype(jnp.int32).reshape(1)

    pair = pair_rows(requests, shift_along(requests, 0, 0, 1))
    lines = spread(pair, 2)
    own, staged = project_own(node_feats, weight)
    low, high = project(own, spread(node_feats, 0)[1:], staged, lines[1:])
    left_low = shift_along(low, 1, 1)
    right_high = shift_along(high, 1, 3)
    left_high = shift_along(high, 1, 1)
    right_low = shift_along(low, 1, 3)
    far_low = shift_along(left_low, 1, 1)
    far_high = shift_along(right_high, 1, 3)
    planes = [low, high, left_low, left_high, far_low, far_high, right_low, right_high]
    own_blocks = own.reshape(num_blocks, rows, feats)

    masks = stage_masks(tile_count, tile_masks)
    lists, spots = ready(device, tile_dst, tile_src, tile_count)
    ratio, init, peak, att3, picks = prep(own_blocks, att_src, att_dst)

    held = lax.optimization_barrier((planes, lines, ratio, init, peak, att3, picks, lists, spots, masks))
    planes, lines, ratio, init, peak, att3, picks, lists, spots, masks = held
    picked = pick_blocks(device, lines, planes)
    arrived = {(hop, half): picked[2 * hop + half] for hop in range(SIDE) for half in range(2)}
    arrived[0, 1] = shift_along(arrived[0, 1], 2, 0, 1)
    for hop, half in ((2, 0), (2, 1), (1, 0), (3, 0), (1, 1), (3, 1)):
        arrived[hop, half] = shift_along(arrived[hop, half], 2, hop, half)
    landed = [[arrived[key] for key in keys] for keys in GROUPS]

    acc, top = init, peak
    for part in range(len(GROUPS) - 1):
        acc, top = attend_step(part, lists, masks, ratio, acc, top, att3, picks, landed[part])
    out = attend_last(
        lists,
        masks,
        ratio,
        acc,
        top,
        att3,
        picks,
        out_bias.reshape(1, feats),
        (tile_dst, spots, tile_count),
        (att_src, att_dst),
        own_blocks,
        sum(landed[:-1], []),
        landed[-1],
    )
    return out.reshape(num_blocks * rows, feats)


def solution(mesh):
    placed = (
        P("node", None),
        P(),
        P(),
        P(),
        P(),
        P("node", None),
        P("node", None),
        P("node", None),
        P("node", None, None, None),
        P("node"),
    )
    return jax.shard_map(
        local, mesh=mesh, in_specs=placed, out_specs=P("node", None), check_vma=False
    )
```
